32 devices in a mesh: section: 2 (over core), group: 4 (over y, x), expert: 4 (over z).
Axes of the slice: x: 2, y: 2, z: 4, core: 2. Of those that a mesh axis runs over, the one named last changes fastest.
Arguments:
- tokens: bfloat16 [8, 256, 2048], P('group', 'expert'), parts along dimension 0
- chosen: int32 [2, 8, 1, 4], P('section', 'group'), parts along dimension 1, may hold values from 0 to 255, as said below
- norm_gain: float32 [2, 2048], P('section'), may hold values from 0.25 to 1.75
- router: bfloat16 [2, 2048, 1], P('section'), may hold values from -0.25 to 0.25
- w_in: bfloat16 [2, 4, 2048, 2048], P('section', 'expert'), may hold values from -0.125 to 0.125
- w_out: bfloat16 [2, 4, 2048, 2048], P('section', 'expert'), may hold values from -0.0625 to 0.0625
Outputs:
- outputs: bfloat16 [2, 8, 256, 2048], P('section', 'group', 'expert'), parts along dimension 1
The draws below stay inside these ranges and needn't reach their ends.
There are 4 independent parts, one for each index of `group`. The reference program is written for one: setup_inputs(seed, part) draws one part's arguments, and reference() takes and returns one part's arrays. A program takes and returns all parts, laid end to end along the dimension named above; an argument that names none is the same for every part. Nothing has to cross between parts.
Inputs may be any that keep to these rules, and one draw needn't show every extreme that they name: `chosen`: for each section, micro-batch and expert the 4 indices are distinct and in no particular order. Of one device's tokens (an aligned block of 64 indices) an expert chooses at most 2; in every draw some expert chooses exactly 2 from some block.
All inputs are finite; a program needn't handle non-finite values.
Results may differ from the reference program's by a relative error of at most 0.001.
Values may be sent and summed in bfloat16 or wider, within the bound.
A program may use at most 64 MiB of HBM per device.

```python
import math
import jax
import jax.numpy as jnp
from jax import lax

D = 2048
FF = 8192
TOK_DEV = 64
MICRO = 2
SLOT = 2
EXPERTS = 1
SPLIT = 4
TOK_MB = 256
CAP = 4
N_SECTION = 2
N_EXPERT = 4


def draw_tokens(key, part):
    key_base, key_rows, key_cols = jax.random.split(key, 3)
    shape = (MICRO, TOK_MB, D)
    base = jax.random.normal(key_base, shape, jnp.float32)
    row_scale = jnp.exp(jax.random.uniform(key_rows, (MICRO, TOK_MB, 1), jnp.float32, math.log(0.3), math.log(3.0)))
    col_scale = jnp.exp(jax.random.uniform(key_cols, (D,), jnp.float32, -math.log(2.0), math.log(2.0)))
    return (base * row_scale * col_scale).astype(jnp.bfloat16)


def chosen_list(key):
    key_order, key_shift, key_score, key_shuffle = jax.random.split(key, 4)
    half_slot = SLOT // 2
    order = jax.random.permutation(key_order, N_EXPERT)
    shifts = jax.random.randint(key_shift, (N_EXPERT // 2,), -half_slot, half_slot + 1)
    shifts = shifts.at[0].set(half_slot)
    paired = jnp.stack([half_slot + shifts, half_slot - shifts], axis=1).reshape(N_EXPERT)
    counts = jnp.zeros((N_EXPERT,), jnp.int32).at[order].set(paired.astype(jnp.int32))
    scores = jax.random.randint(key_score, (N_EXPERT, TOK_DEV), 0, 1 << 20) * 1024 + jnp.arange(TOK_DEV, dtype=jnp.int32)[None, :]
    ranks = jnp.argsort(jnp.argsort(scores, axis=1, stable=True), axis=1, stable=True)
    picked = ranks < counts[:, None]
    positions = jnp.nonzero(picked.reshape(-1), size=CAP)[0].astype(jnp.int32)
    shuffle = jax.random.permutation(key_shuffle, CAP)
    return positions[shuffle].astype(jnp.int32)


def draw_chosen(key, part):
    keys = jax.random.split(jax.random.fold_in(key, 7), N_SECTION * MICRO * EXPERTS)
    lists = jax.vmap(chosen_list)(keys)
    return lists.reshape(N_SECTION, MICRO, EXPERTS, CAP).astype(jnp.int32)


def block_scale(key, dims, cuts, smallest, high):
    def one(dim, shards_of):
        heights = jax.random.uniform(jax.random.fold_in(jax.random.fold_in(key, 6), dim), (shards_of,), jnp.float32, smallest / len(cuts), high / len(cuts))
        return jnp.repeat(jnp.exp(heights), dims[dim] // shards_of).reshape((-1,) + (1,) * (len(dims) - dim - 1))

    gain = one(*cuts[0])
    for cut in cuts[1:]:
        gain = gain * one(*cut)
    return gain


def scatter_about(key, extent, spread, bound, shards=(), kind=jnp.bfloat16):
    level = block_scale(key, extent, shards, -0.22, 0.18) if shards else 1.0
    values = jax.random.normal(key, extent, jnp.float32) * spread * level
    return jnp.minimum(jnp.maximum(values, -bound), bound).astype(kind)


def setup_inputs(seed: int = 0, part: int = 0) -> dict:
    splits = jax.random.split(jax.random.key(seed), 7)
    part_splits = jax.random.split(jax.random.fold_in(splits[6], part), 7)
    tokens = draw_tokens(jax.random.fold_in(jax.random.fold_in(splits[6], part), 71), part)
    chosen = draw_chosen(jax.random.fold_in(jax.random.fold_in(splits[6], part), 71), part)
    norm_gain = jnp.clip(1.0 + 0.15 * jax.random.normal(splits[2], (N_SECTION, D), jnp.float32), 0.25, 1.75)
    router = scatter_about(splits[3], (N_SECTION, D, EXPERTS), (D // 4) ** -0.5, 0.25, ((0, 2),))
    w_in = scatter_about(splits[4], (N_SECTION, N_EXPERT, D, FF // SPLIT), D ** -0.5, 0.125, ((0, 2), (1, 4)))
    w_out = scatter_about(splits[5], (N_SECTION, N_EXPERT, FF // SPLIT, D), FF ** -0.5, 0.0625, ((0, 2), (1, 4)))
    return {"tokens": tokens, "chosen": chosen, "norm_gain": norm_gain, "router": router, "w_in": w_in, "w_out": w_out}


def expert_layer(act, gain_row, router_cols, w_first, w_second, chosen_now):
    floats = act.astype(jnp.float32)
    inverse_rms = lax.rsqrt(lax.optimization_barrier(jnp.mean(floats * floats, axis=-1, keepdims=True)) + 1e-06)
    normed = (floats * inverse_rms * gain_row).astype(jnp.bfloat16)
    gate_all = jax.nn.sigmoid(jnp.dot(normed, router_cols, preferred_element_type=jnp.float32))
    hidden_each = FF // SPLIT
    w_first_all = w_first.reshape(EXPERTS, SPLIT, D, hidden_each).transpose(0, 2, 1, 3).reshape(EXPERTS, D, FF)
    w_second_all = w_second.reshape(EXPERTS, FF, D)

    def one_expert(items):
        first_mat, second_mat, token_ids, column = items
        picked = normed[token_ids]
        hidden = jax.nn.gelu(jnp.dot(picked, first_mat, preferred_element_type=jnp.float32), approximate=True).astype(jnp.bfloat16)
        result = jnp.dot(hidden, second_mat, preferred_element_type=jnp.float32)
        weights = gate_all[token_ids, column]
        return result * weights[:, None]
    results = lax.map(one_expert, (w_first_all, w_second_all, chosen_now, jnp.arange(EXPERTS, dtype=jnp.int32)))
    combined = jnp.zeros((TOK_MB, D), jnp.float32).at[chosen_now.reshape(-1)].add(results.reshape(-1, D))
    return (floats + combined).astype(jnp.bfloat16)

def reference(tokens, chosen, norm_gain, router, w_in, w_out):
    section_rows = []
    previous = [tokens[batch_at] for batch_at in range(MICRO)]
    for section_at in range(N_SECTION):
        current = []
        for batch_at in range(MICRO):
            layer_out = expert_layer(previous[batch_at], norm_gain[section_at], router[section_at], w_in[section_at], w_out[section_at], chosen[section_at, batch_at])
            current.append(layer_out)
        section_rows.append(jnp.stack(current))
        previous = current
    return jnp.stack(section_rows)
```

```python
import functools

import jax
import jax.numpy as jnp
from jax import lax
from jax.experimental import pallas as pl
from jax.experimental.pallas import tpu as pltpu
from jax.sharding import PartitionSpec as P

F32 = jnp.float32
BF16 = jnp.bfloat16
EPS = 1e-06
PARTS = 3


def row_iota(shape):
    return lax.broadcasted_iota(jnp.int32, shape, 0)


def lane_iota(shape):
    return lax.broadcasted_iota(jnp.int32, shape, 1)


def split_three(value):
    high = value.astype(BF16)
    rest = value - high.astype(F32)
    mid = rest.astype(BF16)
    low = (rest - mid.astype(F32)).astype(BF16)
    return jnp.concatenate([high, mid, low], axis=0)


def relay_kernel(
    dims,
    tok_hbm,
    chosen_hbm,
    gain_hbm,
    router_hbm,
    w1_hbm,
    w2_hbm,
    out_v,
    chosen_ref,
    gain_ref,
    router_ref,
    tok_v,
    w1_v,
    w2_v,
    rows_buf,
    x_v,
    acc_v,
    hid_v,
    part_send,
    part_recv,
    part_last,
    c_v,
    c_recv,
    ids_send,
    ids_recv,
    rows_rsem,
    part_rsem,
    misc_rsem,
    small_sem,
    tok_sem,
    w1_sem,
    w2_sem,
    rows_ssem,
    part_ssem,
    misc_ssem,
):
    micro, tok_rows, width, owners, cap, chunks, step = dims
    rows = micro * cap
    total = owners * tok_rows
    section = lax.axis_index("section")
    me = lax.axis_index("expert")

    def copy_to(src, dst, ssem, rsem, sec, exp):
        return pltpu.make_async_remote_copy(
            src_ref=src,
            dst_ref=dst,
            send_sem=ssem,
            recv_sem=rsem,
            device_id={"section": sec, "expert": exp},
            device_id_type=pl.DeviceIdType.MESH,
        )

    def all_of(ref, sem):
        return pltpu.make_async_copy(ref, ref, sem)

    def peer(k):
        low = k + jnp.where(k >= me, 1, 0)
        top = owners - 1 - k
        high = top - jnp.where(top <= me, 1, 0)
        return jnp.where(2 * me < owners, high, low)

    barrier = pltpu.get_barrier_semaphore()
    for o in range(1, owners):
        pl.semaphore_signal(
            barrier,
            inc=1,
            device_id={"section": section, "expert": lax.rem(me + o, owners)},
            device_id_type=pl.DeviceIdType.MESH,
        )
    for o in range(owners):
        pl.semaphore_signal(
            barrier,
            inc=1,
            device_id={"section": 1 - section, "expert": lax.rem(me + o, owners)},
            device_id_type=pl.DeviceIdType.MESH,
        )
    tok_copies = [
        pltpu.make_async_copy(
            tok_hbm.at[m], tok_v.at[pl.ds(m * tok_rows, tok_rows)], tok_sem.at[m]
        )
        for m in range(micro)
    ]
    small_copies = [
        pltpu.make_async_copy(chosen_hbm, chosen_ref, small_sem.at[0]),
        pltpu.make_async_copy(gain_hbm, gain_ref, small_sem.at[1]),
        pltpu.make_async_copy(router_hbm, router_ref, small_sem.at[2]),
    ]
    for c in small_copies[:1] + tok_copies + small_copies[1:]:
        c.start()
    w1_copies = [
        pltpu.make_async_copy(
            w1_hbm.at[0, 0, pl.ds(k * step, step)], w1_v.at[pl.ds(k * step, step)], w1_sem.at[k]
        )
        for k in range(chunks)
    ]
    w2_copies = [
        pltpu.make_async_copy(
            w2_hbm.at[0, 0, :, pl.ds(k * step, step)], w2_v.at[k], w2_sem.at[k]
        )
        for k in range(chunks)
    ]

    small_copies[0].wait()
    id_col = jnp.full((rows, 128), -1, jnp.int32)
    id_row = jnp.full((rows, 128), -1, jnp.int32)
    for r in range(rows):
        ident = chosen_ref[0, r // cap, 0, r % cap] + (r // cap) * total
        id_col = jnp.where(row_iota((rows, 128)) == r, ident, id_col)
        lanes = lane_iota((rows, 128))
        for part in range(PARTS):
            id_row = jnp.where(lanes == part * rows + r, ident, id_row)
    ids_send[...] = id_row

    def own_ids(iota):
        value = iota + me * tok_rows
        for m in range(1, micro):
            value = value + jnp.where(iota >= m * tok_rows, total - tok_rows, 0)
        return value

    for c in tok_copies:
        c.wait()
    for c in w1_copies + w2_copies:
        c.start()
    mine = own_ids(lane_iota((rows, micro * tok_rows)))
    onehot = (mine == id_col[:, :1]).astype(F32).astype(BF16)
    rows_buf[me] = jnp.dot(onehot, tok_v[...], preferred_element_type=F32).astype(BF16)
    pl.semaphore_wait(barrier, 2 * owners - 1)

    row_copies = [
        copy_to(
            rows_buf.at[me], rows_buf.at[me], rows_ssem, rows_rsem, section, peer(k)
        )
        for k in range(owners - 1)
    ]

    def gathered_rows():
        all_of(rows_buf.at[pl.ds(0, owners - 1)], rows_rsem).wait()
        value = rows_buf[0].astype(F32)
        for p in range(1, owners):
            value = value + rows_buf[p].astype(F32)
        return value

    def placed(base, ids_row, contrib):
        mine = own_ids(row_iota((micro * tok_rows, PARTS * rows)))
        hit = (mine == ids_row[:1, : PARTS * rows]).astype(F32).astype(BF16)
        added = jnp.dot(hit, split_three(contrib), preferred_element_type=F32)
        return (base.astype(F32) + added).astype(BF16)

    def second_matmul(j, gate):
        w2_copies[j].wait()
        return (
            jnp.dot(hid_v[...], w2_v[j], preferred_element_type=F32) * gate
        ).astype(BF16)

    @pl.when(section == 0)
    def _():
        for c in row_copies:
            c.start()
        all_of(rows_buf.at[pl.ds(0, owners - 1)], rows_ssem).wait()
        ids_copy = copy_to(ids_send, ids_recv, misc_ssem.at[0], misc_rsem.at[0], 1, me)
        ids_copy.start()
        for c in small_copies[1:]:
            c.wait()
        floats = gathered_rows()
        inverse = lax.rsqrt(jnp.mean(floats * floats, axis=-1, keepdims=True) + EPS)
        normed = (floats * inverse * gain_ref[...]).astype(BF16)
        x_v[...] = normed
        score = jnp.sum(normed.astype(F32) * router_ref[...].astype(F32), axis=-1, keepdims=True)
        gate = jax.nn.sigmoid(score)
        for k in range(chunks):
            w1_copies[k].wait()
            piece = jnp.dot(
                x_v[:, k * step : (k + 1) * step],
                w1_v[k * step : (k + 1) * step, :],
                preferred_element_type=F32,
            )
            acc_v[...] = piece if k == 0 else acc_v[...] + piece
        hid_v[...] = jax.nn.gelu(acc_v[...], approximate=True).astype(BF16)
        for j in range(chunks):
            part_send[j] = second_matmul(j, gate)
            for p in [peer(k) for k in range(owners - 1)] + [me]:
                copy_to(
                    part_send.at[j], part_recv.at[j, me], part_ssem, part_rsem.at[j], 1, p
                ).start()
        back = copy_to(c_v, c_recv, misc_ssem.at[1], misc_rsem.at[1], 0, me)
        back.wait_recv()
        out_v[...] = placed(tok_v[...], id_row, c_recv[...])
        all_of(part_recv, part_ssem).wait()
        ids_copy.wait_send()

    @pl.when(section != 0)
    def _():
        copy_to(ids_send, ids_recv, misc_ssem.at[0], misc_rsem.at[0], 1, me).wait_recv()
        for c in row_copies:
            c.start()
        all_of(rows_buf.at[pl.ds(0, owners - 1)], rows_ssem).wait()
        for c in small_copies[1:]:
            c.wait()
        raw = gathered_rows()
        before = ids_recv[...]
        match = ((id_col == before) & (lane_iota((rows, 128)) < rows)).astype(F32)
        for c in w1_copies:
            c.wait()
        squares = jnp.zeros((rows, 128), F32)
        scores = jnp.zeros((rows, 128), F32)
        for k in range(chunks):
            all_of(part_recv.at[k], part_rsem.at[k]).wait()
            span = slice(k * step, (k + 1) * step)
            contrib = part_recv[k, 0].astype(F32)
            for p in range(1, owners):
                contrib = contrib + part_recv[k, p].astype(F32)
            c_v[:, span] = contrib
            act = raw[:, span]
            added = match[:, 0:1] * contrib[0:1, :]
            for r in range(1, rows):
                added = added + match[:, r : r + 1] * contrib[r : r + 1, :]
            act = (act + added).astype(BF16).astype(F32)
            scaled = (act * gain_ref[:, span]).astype(BF16)
            weighted = scaled.astype(F32) * router_ref[:, span].astype(F32)
            square = act * act
            for b in range(step // 128):
                squares = squares + square[:, b * 128 : (b + 1) * 128]
                scores = scores + weighted[:, b * 128 : (b + 1) * 128]
            piece = jnp.dot(scaled, w1_v[span, :], preferred_element_type=F32)
            acc_v[...] = piece if k == 0 else acc_v[...] + piece
        back = copy_to(c_v, c_recv, misc_ssem.at[1], misc_rsem.at[1], 0, me)
        back.start()
        inverse = lax.rsqrt(jnp.sum(squares, axis=-1, keepdims=True) / width + EPS)
        gate = jax.nn.sigmoid(jnp.sum(scores, axis=-1, keepdims=True) * inverse)
        hid_v[...] = jax.nn.gelu(acc_v[...] * inverse, approximate=True).astype(BF16)
        for j in range(chunks):
            part_send[j] = second_matmul(j, gate)
            for k in range(owners - 1):
                copy_to(
                    part_send.at[j], part_last.at[j, me], part_ssem, part_rsem.at[chunks + j],
                    1, peer(k),
                ).start()
            part_last[j, me] = part_send[j]
        out_v[...] = placed(tok_v[...], before, c_v[...])
        for j in range(chunks):
            span = slice(j * step, (j + 1) * step)
            all_of(part_last.at[j, pl.ds(0, owners - 1)], part_rsem.at[chunks + j]).wait()
            contrib = part_last[j, 0].astype(F32)
            for p in range(1, owners):
                contrib = contrib + part_last[j, p].astype(F32)
            out_v[:, span] = placed(out_v[:, span], id_row, contrib)
        all_of(part_last.at[:, pl.ds(0, owners - 1)], part_ssem).wait()
        back.wait_send()


def scoped_kernel(dims, *refs):
    micro, chunks = dims[0], dims[5]
    dma = pltpu.SemaphoreType.DMA

    pl.run_scoped(
        lambda *sems: relay_kernel(dims, *refs, *sems),
        dma((3,)),
        dma((micro,)),
        dma((chunks,)),
        dma((chunks,)),
        dma,
        dma,
        dma((2,)),
    )


def fused(tokens, chosen, norm_gain, router, w_in, w_out):
    micro, tok_rows, width = tokens.shape
    owners = lax.axis_size("expert")
    cap = chosen.shape[3]
    hidden = w_in.shape[3]
    rows = micro * cap
    chunks = 4
    step = width // chunks
    dims = (micro, tok_rows, width, owners, cap, chunks, step)
    vmem = pl.BlockSpec(memory_space=pltpu.VMEM)
    hbm = pl.BlockSpec(memory_space=pltpu.HBM)
    dma = pltpu.SemaphoreType.DMA
    result = pl.pallas_call(
        functools.partial(scoped_kernel, dims),
        out_shape=pltpu.VMEM((micro * tok_rows, width), BF16),
        in_specs=[hbm] * 6,
        out_specs=vmem,
        scratch_shapes=[
            pltpu.SMEM((1, micro, 1, cap), jnp.int32),
            pltpu.VMEM((1, width), F32),
            pltpu.VMEM((1, width), BF16),
            pltpu.VMEM((micro * tok_rows, width), BF16),
            pltpu.VMEM((width, hidden), BF16),
            pltpu.VMEM((chunks, hidden, step), BF16),
            pltpu.VMEM((owners, rows, width), BF16),
            pltpu.VMEM((rows, width), BF16),
            pltpu.VMEM((rows, hidden), F32),
            pltpu.VMEM((rows, hidden), BF16),
            pltpu.VMEM((chunks, rows, step), BF16),
            pltpu.VMEM((chunks, owners, rows, step), BF16),
            pltpu.VMEM((chunks, owners, rows, step), BF16),
            pltpu.VMEM((rows, width), F32),
            pltpu.VMEM((rows, width), F32),
            pltpu.VMEM((rows, 128), jnp.int32),
            pltpu.VMEM((rows, 128), jnp.int32),
            dma,
            dma((2 * chunks,)),
            dma((2,)),
        ],
        compiler_params=pltpu.CompilerParams(
            collective_id=0, has_side_effects=True, vmem_limit_bytes=60 * 1024 * 1024
        ),
    )(tokens, chosen, norm_gain, router[:, :, 0], w_in, w_out)
    return result.reshape(1, micro, tok_rows, width)


def passed_along(value, axis, steps):
    count = lax.axis_size(axis)
    leading, last = (max(0, -steps), min(count, count - steps))
    return lax.ppermute(value, axis, [(source, source + steps) for source in range(leading, last)])


def moe_layer(
    current, picks_now, gain_row, router_cols, w_first, w_second, device, owners, shards_each
):
    tok_rows, width = current.shape
    experts, capacity = picks_now.shape
    slots = 2 * capacity // owners
    floats = current.astype(jnp.float32)
    inverse_rms = lax.rsqrt(jnp.mean(floats * floats, axis=-1, keepdims=True) + 1e-06)
    normed = (floats * inverse_rms * gain_row).astype(jnp.bfloat16)
    gate_all = jax.nn.sigmoid(jnp.dot(normed, router_cols, preferred_element_type=jnp.float32))
    owner_of = picks_now // tok_rows
    onehot = (owner_of[:, :, None] == jnp.arange(owners, dtype=jnp.int32)[None, None, :]).astype(
        jnp.int32
    )
    order_slot = jnp.cumsum(onehot, axis=1) - 1
    slot_of = jnp.sum(order_slot * onehot, axis=2)
    is_mine = owner_of == device
    local_idx = picks_now - device * tok_rows
    slot_hit = (
        (slot_of[:, :, None] == jnp.arange(slots, dtype=jnp.int32)[None, None, :])
        & is_mine[:, :, None]
    ).astype(jnp.float32)
    tok_hit = (
        local_idx[:, :, None] == jnp.arange(tok_rows, dtype=jnp.int32)[None, None, :]
    ).astype(jnp.float32)
    selector = jnp.einsum("xcs,xct->xst", slot_hit, tok_hit)
    flat_select = selector.reshape(experts * slots, tok_rows)
    gate_slot = jnp.einsum("xst,tx->xs", selector, gate_all, precision=lax.Precision.HIGHEST)
    dispatched = jnp.dot(
        flat_select.astype(jnp.bfloat16), normed, preferred_element_type=jnp.float32
    ).astype(jnp.bfloat16)
    outgoing = jnp.broadcast_to(
        dispatched.reshape(experts, 1, slots, width), (experts, shards_each, slots, width)
    ).reshape(owners, slots, width)
    arrived = lax.all_to_all(outgoing, "expert", split_axis=0, concat_axis=0, tiled=True)
    item_count = arrived.shape[1]
    flat_rows = arrived.reshape(-1, width)
    hidden = jax.nn.gelu(
        jnp.dot(flat_rows, w_first, preferred_element_type=jnp.float32), approximate=True
    ).astype(jnp.bfloat16)
    partial_value = jnp.dot(hidden, w_second, preferred_element_type=jnp.float32).reshape(
        owners, item_count, width
    )
    returned = lax.all_to_all(partial_value, "expert", split_axis=0, concat_axis=0, tiled=True)
    summed = returned.reshape(experts, shards_each, slots, width).sum(axis=1)
    weighted = summed * gate_slot[:, :, None]
    contrib = jnp.dot(
        flat_select.T, weighted.reshape(experts * slots, width), precision=lax.Precision.HIGHEST
    )
    return (floats + contrib).astype(jnp.bfloat16)


def fits(tokens, chosen, w_in, sections, owners):
    micro, tok_rows, width = tokens.shape
    experts, cap = chosen.shape[2:]
    rows = micro * cap
    whole_tiles = rows % 8 == 0 and width % 512 == 0 and w_in.shape[3] % 256 == 0
    return sections == 2 and experts == 1 and whole_tiles and rows * PARTS <= 128 and owners <= 8


def local(tokens, chosen, norm_gain, router, w_in, w_out):
    sections = lax.axis_size("section")
    owners = lax.axis_size("expert")
    if fits(tokens, chosen, w_in, sections, owners):
        return fused(tokens, chosen, norm_gain, router, w_in, w_out)
    section_index = lax.axis_index("section")
    device = lax.axis_index("expert")
    micro_count, tok_rows, width = tokens.shape
    experts = chosen.shape[2]
    shards_each = owners // experts
    gain_row = norm_gain[0]
    router_cols = router[0]
    w_first = w_in[0, 0]
    w_second = w_out[0, 0]
    outputs = jnp.zeros((1, micro_count, tok_rows, width), jnp.bfloat16)
    received = jnp.zeros((tok_rows, width), jnp.bfloat16)
    tick_count = micro_count + sections - 1
    for tick_index in range(tick_count):
        batch_index = tick_index - section_index
        clipped = jnp.clip(batch_index, 0, micro_count - 1)
        fresh_input = tokens[min(tick_index, micro_count - 1)]
        current = jnp.where(section_index == 0, fresh_input, received)
        picks_now = lax.dynamic_index_in_dim(chosen[0], clipped, 0, keepdims=False)
        layer_out = moe_layer(
            current,
            picks_now,
            gain_row,
            router_cols,
            w_first,
            w_second,
            device,
            owners,
            shards_each,
        )
        in_range = (batch_index >= 0) & (batch_index < micro_count)
        previous = lax.dynamic_index_in_dim(outputs[0], clipped, 0, keepdims=False)
        written = jnp.where(in_range, layer_out, previous)
        outputs = lax.dynamic_update_index_in_dim(outputs, written[None, None], clipped, 1)
        if tick_index + 1 < tick_count:
            received = passed_along(layer_out, "section", 1)
    return outputs


def solution(mesh):
    placed = (
        P("group", "expert", None),
        P("section", "group", None, None),
        P("section", None),
        P("section", None, None),
        P("section", "expert", None, None),
        P("section", "expert", None, None),
    )
    return jax.shard_map(
        local,
        mesh=mesh,
        in_specs=placed,
        out_specs=P("section", "group", "expert", None),
        check_vma=False,
    )
```

```python
import functools

import jax
import jax.numpy as jnp
from jax import lax
from jax.experimental import pallas as pl
from jax.experimental.pallas import tpu as pltpu
from jax.sharding import PartitionSpec as P

F32 = jnp.float32
BF16 = jnp.bfloat16
EPS = 1e-06
TILE = 256
SEND_TILES = (1, 1, 2, 2, 1, 1)
LAST_TILES = (2, 2, 2, 1, 1)


def row_iota(shape):
    return lax.broadcasted_iota(jnp.int32, shape, 0)


def lane_iota(shape):
    return lax.broadcasted_iota(jnp.int32, shape, 1)


def tile_at(index, count=1):
    return slice(index * TILE, (index + count) * TILE)


def pieces(sizes, tiles):
    found, start = [], 0
    for size in sizes:
        size = min(size, tiles - start)
        if size > 0:
            found.append((start, size))
            start += size
    while start < tiles:
        found.append((start, 1))
        start += 1
    return found


def relay_kernel(
    dims,
    tok_hbm,
    chosen_hbm,
    gain_hbm,
    router_hbm,
    w1_hbm,
    w2_hbm,
    out_v,
    chosen_ref,
    gain_ref,
    router_ref,
    tok_v,
    w1_v,
    w2_v,
    rows_buf,
    xf_v,
    part_send,
    part_recv,
    last_send,
    last_recv,
    c_v,
    c_recv,
    fin_v,
    ids_send,
    ids_recv,
    own_ref,
    rows_rsem,
    part_rsem,
    last_rsem,
    misc_rsem,
    sums,
    outs,
    small_sem,
    tok_sem,
    w1_sem,
    w2_sem,
    rows_ssem,
    part_ssem,
    misc_ssem,
):
    micro, tok_rows, width, hidden, owners, cap, slots = dims
    rows = micro * cap
    each = micro * slots
    items = owners * each
    total = owners * tok_rows
    tokens = micro * tok_rows
    in_tiles, hid_tiles = width // TILE, hidden // TILE
    send_pieces = pieces(SEND_TILES, in_tiles)
    last_pieces = pieces(LAST_TILES, in_tiles)
    section = lax.axis_index("section")
    me = lax.axis_index("expert")

    def copy_to(src, dst, ssem, rsem, sec, exp):
        return pltpu.make_async_remote_copy(
            src_ref=src,
            dst_ref=dst,
            send_sem=ssem,
            recv_sem=rsem,
            device_id={"section": sec, "expert": exp},
            device_id_type=pl.DeviceIdType.MESH,
        )

    def all_of(ref, sem):
        return pltpu.make_async_copy(ref, ref, sem)

    def peer(k):
        low = k + jnp.where(k >= me, 1, 0)
        top = owners - 1 - k
        high = top - jnp.where(top <= me, 1, 0)
        return jnp.where(2 * me < owners, high, low)

    staged = [0, 0]

    def multiply(acc, lhs, rhs, unit):
        register = staged[unit]
        staged[unit] = 1 - register
        pltpu.matmul_push_rhs(rhs, staging_register=register, mxu_index=unit)
        pltpu.matmul_acc_lhs(acc, lhs, load_staged_rhs=register)

    barrier = pltpu.get_barrier_semaphore()
    for o in range(1, owners):
        pl.semaphore_signal(
            barrier,
            inc=1,
            device_id={"section": section, "expert": lax.rem(me + o, owners)},
            device_id_type=pl.DeviceIdType.MESH,
        )
    for o in range(owners):
        pl.semaphore_signal(
            barrier,
            inc=1,
            device_id={"section": 1 - section, "expert": lax.rem(me + o, owners)},
            device_id_type=pl.DeviceIdType.MESH,
        )
    tok_copies = [
        pltpu.make_async_copy(
            tok_hbm.at[m], tok_v.at[pl.ds(m * tok_rows, tok_rows)], tok_sem.at[m]
        )
        for m in range(micro)
    ]
    small_copies = [
        pltpu.make_async_copy(chosen_hbm, chosen_ref, small_sem.at[0]),
        pltpu.make_async_copy(gain_hbm, gain_ref, small_sem.at[1]),
        pltpu.make_async_copy(router_hbm, router_ref, small_sem.at[2]),
    ]
    for c in small_copies[:1] + tok_copies + small_copies[1:]:
        c.start()
    parts = 4
    deep, half = width // parts, width // 2
    w1_copies = [
        pltpu.make_async_copy(
            w1_hbm.at[0, 0, pl.ds(k * deep, deep)], w1_v.at[pl.ds(k * deep, deep)], w1_sem
        )
        for k in range(parts)
    ]
    w2_copies = [
        pltpu.make_async_copy(
            w2_hbm.at[0, 0, :, pl.ds(k * half, half)],
            w2_v.at[:, pl.ds(k * half, half)],
            w2_sem.at[k],
        )
        for k in range(2)
    ]
    if tokens < TILE:
        tok_v[tokens:, :] = jnp.zeros((TILE - tokens, width), BF16)

    small_copies[0].wait()
    id_col = jnp.full((rows, 128), -1, jnp.int32)
    code_col = jnp.full((rows, 128), -1, jnp.int32)
    item_id = jnp.full((items, 128), -1, jnp.int32)
    own_id = jnp.full((items, 128), -1, jnp.int32)
    for m in range(micro):
        owner_of = []
        for c in range(cap):
            r = m * cap + c
            pick = chosen_ref[0, m, 0, c]
            ident = pick + m * total
            owner = lax.div(pick, jnp.int32(tok_rows))
            slot = jnp.int32(0)
            for earlier in owner_of:
                slot = slot + jnp.where(earlier == owner, 1, 0)
            owner_of.append(owner)
            inner = m * slots + slot
            id_col = jnp.where(row_iota((rows, 128)) == r, ident, id_col)
            code_col = jnp.where(row_iota((rows, 128)) == r, owner * slots + slot, code_col)
            item_id = jnp.where(row_iota((items, 128)) == owner * each + inner, ident, item_id)
            at = jnp.where(owner == me, inner, -1)
            own_id = jnp.where(row_iota((items, 128)) == at, ident, own_id)
    ids_send[...] = id_col
    own_ref[...] = own_id

    lanes = lane_iota((items, TILE))
    lane_id = lanes + me * tok_rows
    for m in range(1, micro):
        lane_id = lane_id + jnp.where(lanes >= m * tok_rows, total - tok_rows, 0)
    lane_id = jnp.where(lanes < tokens, lane_id, -2)
    pick_lhs = (
        (lane_id == jnp.concatenate([own_id] * (TILE // 128), axis=1)).astype(F32).astype(BF16)
    )

    for c in tok_copies:
        c.wait()
    for c in w1_copies + w2_copies:
        c.start()

    def pick_rows(first, count):
        for n in range(first, first + count):
            multiply(sums[n], pick_lhs, tok_v[:, tile_at(n)], n % 2)
        for n in range(first, first + count):
            rows_buf[me, :, tile_at(n)] = pltpu.matmul_pop(sums[n])[:each].astype(BF16)

    def row_sends(first, count):
        span = tile_at(first, count)
        return [
            copy_to(
                rows_buf.at[me, :, span], rows_buf.at[me, :, span], rows_ssem, rows_rsem,
                section, peer(k),
            )
            for k in range(owners - 1)
        ]

    def gathered_rows():
        all_of(rows_buf.at[pl.ds(0, owners - 1)], rows_rsem).wait()
        for p in range(owners):
            xf_v[p * each : (p + 1) * each, :] = rows_buf[p].astype(F32)

    def folded(value, start):
        for b in range(TILE // 128):
            start = start + value[:, b * 128 : (b + 1) * 128]
        return start

    def scaled_tile(act, tile, stats):
        span = tile_at(tile)
        scaled = (act * gain_ref[:, span]).astype(BF16)
        weighted = scaled.astype(F32) * router_ref[:, span].astype(F32)
        return scaled, (folded(act * act, stats[0]), folded(weighted, stats[1]))

    def closing(stats):
        inverse = lax.rsqrt(jnp.sum(stats[0], axis=-1, keepdims=True) / width + EPS)
        score = jnp.sum(stats[1], axis=-1, keepdims=True)
        gate = jax.nn.sigmoid(jnp.where(inverse > 0, score * inverse, 0.0))
        return inverse, gate

    hid = {}

    def finish(pair, inverse):
        for n in (2 * pair, 2 * pair + 1):
            value = jnp.where(inverse > 0, pltpu.matmul_pop(sums[n]) * inverse, 0.0)
            hid[n] = jax.nn.gelu(value, approximate=True).astype(BF16)

    def second_matmul(inverse, done, emit):
        pairs = hid_tiles // 2
        for t in range(in_tiles):
            if t == in_tiles // 2:
                w2_copies[1].wait()
            for i in range(pairs):
                if t == 0 and i >= done:
                    finish(i, inverse)
                for unit in range(2):
                    k = 2 * i + unit
                    multiply(outs[t % 3][unit], hid[k], w2_v[tile_at(k), tile_at(t)], unit)
            if t > 0:
                emit(t - 1)
        emit(in_tiles - 1)

    def popped(t):
        return pltpu.matmul_pop(outs[t % 3][0]) + pltpu.matmul_pop(outs[t % 3][1])

    def place(base_ref, ids_ref, value_ref, picks, first, count):
        group = 16
        for m in range(micro):
            for g in range(tok_rows // group):
                ids = row_iota((group, 128)) + (m * total + g * group) + me * tok_rows
                masks = [(ids == ids_ref[r : r + 1, :], r) for r in picks(m)]
                at = slice(m * tok_rows + g * group, m * tok_rows + (g + 1) * group)
                for b in range(first * TILE // 128, (first + count) * TILE // 128):
                    span = slice(b * 128, (b + 1) * 128)
                    added = jnp.zeros((group, 128), F32)
                    for mask, r in masks:
                        added = jnp.where(mask, value_ref[r : r + 1, span], added)
                    out_v[at, span] = (base_ref[at, span].astype(F32) + added).astype(BF16)

    def whole_picks(m):
        return range(m * cap, (m + 1) * cap)

    def slot_picks(m):
        return range(m * slots, (m + 1) * slots)

    near = in_tiles // 2
    zero = jnp.zeros((items, 128), F32)

    @pl.when(section == 0)
    def _():
        pick_rows(0, near)
        pl.semaphore_wait(barrier, 2 * owners - 1)
        for c in row_sends(0, near):
            c.start()
        pick_rows(near, in_tiles - near)
        for c in row_sends(near, in_tiles - near):
            c.start()
        for c in small_copies[1:]:
            c.wait()
        all_of(rows_buf.at[pl.ds(0, owners - 1)], rows_ssem).wait()
        ids_copy = copy_to(ids_send, ids_recv, misc_ssem.at[0], misc_rsem.at[0], 1, me)
        ids_copy.start()
        all_of(w1_v, w1_sem).wait()
        w2_copies[0].wait()
        gathered_rows()
        early = row_iota((rows, 128)) < cap
        masks = [code_col == code for code in range(owners * slots)]
        stats = (zero, zero)
        xs = []
        for k in range(in_tiles):
            halves = []
            for b in range(TILE // 128):
                span = slice(k * TILE + b * 128, k * TILE + (b + 1) * 128)
                value = jnp.zeros((rows, 128), F32)
                for p in range(owners):
                    for s in range(slots):
                        q = p * each + s
                        both = xf_v[q : q + 1, span]
                        for m in range(1, micro):
                            after = xf_v[q + m * slots : q + m * slots + 1, span]
                            both = jnp.where(early, both, after)
                        value = jnp.where(masks[p * slots + s], both, value)
                halves.append(value)
            act = jnp.concatenate(halves, axis=1)
            act = jnp.concatenate([act, jnp.zeros((items - rows, TILE), F32)], axis=0)
            scaled, stats = scaled_tile(act, k, stats)
            xs.append(scaled)
        inverse, gate = closing(stats)
        pairs = hid_tiles // 2
        for i in range(pairs):
            for k in range(in_tiles):
                for unit in range(2):
                    n = 2 * i + unit
                    multiply(sums[n], xs[k], w1_v[tile_at(k), tile_at(n)], unit)
            if i > 0:
                finish(i - 1, inverse)

        def emit(t):
            part_send[:, tile_at(t)] = (popped(t)[:rows] * gate[:rows]).astype(BF16)
            for j, (first, count) in enumerate(send_pieces):
                if first + count - 1 == t:
                    span = tile_at(first, count)
                    for p in [peer(k) for k in range(owners - 1)] + [me]:
                        copy_to(
                            part_send.at[:, span], part_recv.at[me, :, span], part_ssem,
                            part_rsem.at[j], 1, p,
                        ).start()

        second_matmul(inverse, pairs - 1, emit)
        back = copy_to(c_v, c_recv, misc_ssem.at[1], misc_rsem.at[1], 0, me)
        back.wait_recv()
        place(tok_v, ids_send, c_recv, whole_picks, 0, in_tiles)
        all_of(part_recv, part_ssem).wait()
        ids_copy.wait_send()

    @pl.when(section != 0)
    def _():
        pick_rows(0, in_tiles)
        pl.semaphore_wait(barrier, 2 * owners - 1)
        copy_to(ids_send, ids_recv, misc_ssem.at[0], misc_rsem.at[0], 1, me).wait_recv()
        for c in row_sends(0, in_tiles):
            c.start()
        for c in small_copies[1:]:
            c.wait()
        all_of(rows_buf.at[pl.ds(0, owners - 1)], rows_ssem).wait()
        gathered_rows()
        early = lax.rem(row_iota((items, 128)), each) < slots
        match = [
            sum((item_id == ids_recv[m * cap + c : m * cap + c + 1, :]).astype(F32) for m in range(micro))
            for c in range(cap)
        ]
        all_of(w1_v, w1_sem).wait()
        w2_copies[0].wait()
        stats = (zero, zero)
        for j, (first, count) in enumerate(send_pieces):
            all_of(part_recv.at[:, :, tile_at(first, count)], part_rsem.at[j]).wait()
            for k in range(first, first + count):
                span = tile_at(k)
                contrib = part_recv[0, :, span].astype(F32)
                for p in range(1, owners):
                    contrib = contrib + part_recv[p, :, span].astype(F32)
                c_v[:, span] = contrib
                halves = []
                for b in range(TILE // 128):
                    inner = slice(k * TILE + b * 128, k * TILE + (b + 1) * 128)
                    act = xf_v[:, inner]
                    for c in range(cap):
                        both = c_v[c : c + 1, inner]
                        for m in range(1, micro):
                            both = jnp.where(early, both, c_v[m * cap + c : m * cap + c + 1, inner])
                        act = act + match[c] * both
                    halves.append(act.astype(BF16).astype(F32))
                scaled, stats = scaled_tile(jnp.concatenate(halves, axis=1), k, stats)
                for n in range(hid_tiles):
                    multiply(sums[n], scaled, w1_v[span, tile_at(n)], n % 2)
        back = copy_to(c_v, c_recv, misc_ssem.at[1], misc_rsem.at[1], 0, me)
        back.start()
        inverse, gate = closing(stats)

        def emit(t):
            value = popped(t) * gate
            for p in range(owners):
                last_send[p, :, tile_at(t)] = value[p * each : (p + 1) * each].astype(BF16)
            for j, (first, count) in enumerate(last_pieces):
                if first + count - 1 == t:
                    span = tile_at(first, count)
                    for p in [peer(k) for k in range(owners - 1)]:
                        copy_to(
                            last_send.at[p, :, span], last_recv.at[me, :, span], part_ssem,
                            last_rsem.at[j], 1, p,
                        ).start()

        second_matmul(inverse, 0, emit)
        place(tok_v, ids_recv, c_v, whole_picks, 0, in_tiles)
        for j, (first, count) in enumerate(last_pieces):
            span = tile_at(first, count)
            all_of(last_recv.at[pl.ds(0, owners - 1), :, span], last_rsem.at[j]).wait()
            value = last_send[me, :, span].astype(F32)
            for k in range(owners - 1):
                value = value + last_recv[peer(k), :, span].astype(F32)
            fin_v[:each, span] = value
            place(out_v, own_ref, fin_v, slot_picks, first, count)
        all_of(last_recv.at[pl.ds(0, owners - 1)], part_ssem).wait()
        back.wait_send()


def scoped_kernel(dims, *refs):
    hidden, width = dims[3], dims[2]
    items = dims[4] * dims[0] * dims[6]
    dma = pltpu.SemaphoreType.DMA
    shape = (items, TILE)
    pl.run_scoped(
        lambda sums, outs, *sems: relay_kernel(dims, *refs, sums, outs, *sems),
        tuple(pltpu.ACC(n % 2)(shape, F32) for n in range(max(hidden, width) // TILE)),
        tuple((pltpu.ACC(0)(shape, F32), pltpu.ACC(1)(shape, F32)) for _ in range(3)),
        dma((3,)),
        dma((dims[0],)),
        dma,
        dma((2,)),
        dma,
        dma,
        dma((2,)),
    )


def fused(tokens, chosen, norm_gain, router, w_in, w_out):
    micro, tok_rows, width = tokens.shape
    owners = lax.axis_size("expert")
    cap = chosen.shape[3]
    hidden = w_in.shape[3]
    rows = micro * cap
    slots = 2 * cap // owners
    each = micro * slots
    items = owners * each
    dims = (micro, tok_rows, width, hidden, owners, cap, slots)
    vmem = pl.BlockSpec(memory_space=pltpu.VMEM)
    hbm = pl.BlockSpec(memory_space=pltpu.HBM)
    dma = pltpu.SemaphoreType.DMA
    result = pl.pallas_call(
        functools.partial(scoped_kernel, dims),
        out_shape=pltpu.VMEM((micro * tok_rows, width), BF16),
        in_specs=[hbm] * 6,
        out_specs=vmem,
        scratch_shapes=[
            pltpu.SMEM((1, micro, 1, cap), jnp.int32),
            pltpu.VMEM((1, width), F32),
            pltpu.VMEM((1, width), BF16),
            pltpu.VMEM((TILE, width), BF16),
            pltpu.VMEM((width, hidden), BF16),
            pltpu.VMEM((hidden, width), BF16),
            pltpu.VMEM((owners, each, width), BF16),
            pltpu.VMEM((items, width), F32),
            pltpu.VMEM((rows, width), BF16),
            pltpu.VMEM((owners, rows, width), BF16),
            pltpu.VMEM((owners, each, width), BF16),
            pltpu.VMEM((owners, each, width), BF16),
            pltpu.VMEM((rows, width), F32),
            pltpu.VMEM((rows, width), F32),
            pltpu.VMEM((8, width), F32),
            pltpu.VMEM((rows, 128), jnp.int32),
            pltpu.VMEM((rows, 128), jnp.int32),
            pltpu.VMEM((items, 128), jnp.int32),
            dma,
            dma((len(pieces(SEND_TILES, width // TILE)),)),
            dma((len(pieces(LAST_TILES, width // TILE)),)),
            dma((2,)),
        ],
        compiler_params=pltpu.CompilerParams(
            collective_id=0, has_side_effects=True, vmem_limit_bytes=60 * 1024 * 1024
        ),
    )(tokens, chosen, norm_gain, router[:, :, 0], w_in, w_out)
    return result.reshape(1, micro, tok_rows, width)


def passed_along(value, axis, steps):
    count = lax.axis_size(axis)
    leading, last = (max(0, -steps), min(count, count - steps))
    return lax.ppermute(value, axis, [(source, source + steps) for source in range(leading, last)])


def moe_layer(
    current, picks_now, gain_row, router_cols, w_first, w_second, device, owners, shards_each
):
    tok_rows, width = current.shape
    experts, capacity = picks_now.shape
    slots = 2 * capacity // owners
    floats = current.astype(jnp.float32)
    inverse_rms = lax.rsqrt(jnp.mean(floats * floats, axis=-1, keepdims=True) + 1e-06)
    normed = (floats * inverse_rms * gain_row).astype(jnp.bfloat16)
    gate_all = jax.nn.sigmoid(jnp.dot(normed, router_cols, preferred_element_type=jnp.float32))
    owner_of = picks_now // tok_rows
    onehot = (owner_of[:, :, None] == jnp.arange(owners, dtype=jnp.int32)[None, None, :]).astype(
        jnp.int32
    )
    order_slot = jnp.cumsum(onehot, axis=1) - 1
    slot_of = jnp.sum(order_slot * onehot, axis=2)
    is_mine = owner_of == device
    local_idx = picks_now - device * tok_rows
    slot_hit = (
        (slot_of[:, :, None] == jnp.arange(slots, dtype=jnp.int32)[None, None, :])
        & is_mine[:, :, None]
    ).astype(jnp.float32)
    tok_hit = (
        local_idx[:, :, None] == jnp.arange(tok_rows, dtype=jnp.int32)[None, None, :]
    ).astype(jnp.float32)
    selector = jnp.einsum("xcs,xct->xst", slot_hit, tok_hit)
    flat_select = selector.reshape(experts * slots, tok_rows)
    gate_slot = jnp.einsum("xst,tx->xs", selector, gate_all, precision=lax.Precision.HIGHEST)
    dispatched = jnp.dot(
        flat_select.astype(jnp.bfloat16), normed, preferred_element_type=jnp.float32
    ).astype(jnp.bfloat16)
    outgoing = jnp.broadcast_to(
        dispatched.reshape(experts, 1, slots, width), (experts, shards_each, slots, width)
    ).reshape(owners, slots, width)
    arrived = lax.all_to_all(outgoing, "expert", split_axis=0, concat_axis=0, tiled=True)
    item_count = arrived.shape[1]
    flat_rows = arrived.reshape(-1, width)
    hidden = jax.nn.gelu(
        jnp.dot(flat_rows, w_first, preferred_element_type=jnp.float32), approximate=True
    ).astype(jnp.bfloat16)
    partial_value = jnp.dot(hidden, w_second, preferred_element_type=jnp.float32).reshape(
        owners, item_count, width
    )
    returned = lax.all_to_all(partial_value, "expert", split_axis=0, concat_axis=0, tiled=True)
    summed = returned.reshape(experts, shards_each, slots, width).sum(axis=1)
    weighted = summed * gate_slot[:, :, None]
    contrib = jnp.dot(
        flat_select.T, weighted.reshape(experts * slots, width), precision=lax.Precision.HIGHEST
    )
    return (floats + contrib).astype(jnp.bfloat16)


def fits(tokens, chosen, w_in, sections, owners):
    micro, tok_rows, width = tokens.shape
    experts, cap = chosen.shape[2:]
    hidden = w_in.shape[3]
    slots = 2 * cap // owners
    whole_tiles = width % 512 == 0 and hidden % 512 == 0 and hidden <= 2048 and width <= 2048
    few = micro == 2 and micro * cap == 8 and owners * micro * slots == 16
    return (
        sections == 2 and experts == 1 and whole_tiles and few
        and tok_rows % 16 == 0 and micro * tok_rows <= TILE
    )


def local(tokens, chosen, norm_gain, router, w_in, w_out):
    sections = lax.axis_size("section")
    owners = lax.axis_size("expert")
    if fits(tokens, chosen, w_in, sections, owners):
        return fused(tokens, chosen, norm_gain, router, w_in, w_out)
    section_index = lax.axis_index("section")
    device = lax.axis_index("expert")
    micro_count, tok_rows, width = tokens.shape
    experts = chosen.shape[2]
    shards_each = owners // experts
    gain_row = norm_gain[0]
    router_cols = router[0]
    w_first = w_in[0, 0]
    w_second = w_out[0, 0]
    outputs = jnp.zeros((1, micro_count, tok_rows, width), jnp.bfloat16)
    received = jnp.zeros((tok_rows, width), jnp.bfloat16)
    tick_count = micro_count + sections - 1
    for tick_index in range(tick_count):
        batch_index = tick_index - section_index
        clipped = jnp.clip(batch_index, 0, micro_count - 1)
        fresh_input = tokens[min(tick_index, micro_count - 1)]
        current = jnp.where(section_index == 0, fresh_input, received)
        picks_now = lax.dynamic_index_in_dim(chosen[0], clipped, 0, keepdims=False)
        layer_out = moe_layer(
            current,
            picks_now,
            gain_row,
            router_cols,
            w_first,
            w_second,
            device,
            owners,
            shards_each,
        )
        in_range = (batch_index >= 0) & (batch_index < micro_count)
        previous = lax.dynamic_index_in_dim(outputs[0], clipped, 0, keepdims=False)
        written = jnp.where(in_range, layer_out, previous)
        outputs = lax.dynamic_update_index_in_dim(outputs, written[None, None], clipped, 1)
        if tick_index + 1 < tick_count:
            received = passed_along(layer_out, "section", 1)
    return outputs


def solution(mesh):
    placed = (
        P("group", "expert", None),
        P("section", "group", None, None),
        P("section", None),
        P("section", None, None),
        P("section", "expert", None, None),
        P("section", "expert", None, None),
    )
    return jax.shard_map(
        local,
        mesh=mesh,
        in_specs=placed,
        out_specs=P("section", "group", "expert", None),
        check_vma=False,
    )
```

```python
import functools

import jax
import jax.numpy as jnp
from jax import lax
from jax.experimental import pallas as pl
from jax.experimental.pallas import tpu as pltpu
from jax.sharding import PartitionSpec as P

F32 = jnp.float32
BF16 = jnp.bfloat16
EPS = 1e-06
TILE = 256
SEND_TILES = (1, 1, 1, 1, 1, 1, 1, 1)
LAST_TILES = (2, 2, 2, 1, 1)


def row_iota(shape):
    return lax.broadcasted_iota(jnp.int32, shape, 0)


def lane_iota(shape):
    return lax.broadcasted_iota(jnp.int32, shape, 1)


def tile_at(index, count=1):
    return slice(index * TILE, (index + count) * TILE)


def pieces(sizes, tiles):
    found, start = [], 0
    for size in sizes:
        size = min(size, tiles - start)
        if size > 0:
            found.append((start, size))
            start += size
    while start < tiles:
        found.append((start, 1))
        start += 1
    return found


def relay_kernel(
    dims,
    tok_hbm,
    chosen_hbm,
    gain_hbm,
    router_hbm,
    w1_hbm,
    w2_hbm,
    out_v,
    chosen_ref,
    gain_ref,
    router_ref,
    tok_v,
    tf_v,
    pick_v,
    w1_v,
    w2_v,
    rows_buf,
    xf_v,
    part_send,
    part_recv,
    last_send,
    last_recv,
    c_v,
    c_recv,
    fin_v,
    ids_send,
    ids_recv,
    own_ref,
    sums,
    outs,
    rows_rsem,
    part_rsem,
    last_rsem,
    misc_rsem,
    small_sem,
    tok_sem,
    w1_sem,
    w2_sem,
    rows_ssem,
    part_ssem,
    misc_ssem,
):
    micro, tok_rows, width, hidden, owners, cap, slots = dims
    rows = micro * cap
    each = micro * slots
    items = owners * each
    total = owners * tok_rows
    tokens = micro * tok_rows
    in_tiles, hid_tiles = width // TILE, hidden // TILE
    send_pieces = pieces(SEND_TILES, in_tiles)
    last_pieces = pieces(LAST_TILES, in_tiles)
    section = lax.axis_index("section")
    me = lax.axis_index("expert")

    def copy_to(src, dst, ssem, rsem, sec, exp):
        return pltpu.make_async_remote_copy(
            src_ref=src,
            dst_ref=dst,
            send_sem=ssem,
            recv_sem=rsem,
            device_id={"section": sec, "expert": exp},
            device_id_type=pl.DeviceIdType.MESH,
        )

    def all_of(ref, sem):
        return pltpu.make_async_copy(ref, ref, sem)

    def peer(k):
        low = k + jnp.where(k >= me, 1, 0)
        top = owners - 1 - k
        high = top - jnp.where(top <= me, 1, 0)
        return jnp.where(2 * me < owners, high, low)

    staged = [0, 0]

    waiting = ([], [])

    def push(rhs, unit):
        register = staged[unit]
        staged[unit] = 1 - register
        pltpu.matmul_push_rhs(rhs, staging_register=register, mxu_index=unit)
        waiting[unit].append(register)

    def multiply(acc, lhs, rhs, unit):
        if rhs is not None:
            push(rhs, unit)
        pltpu.matmul_acc_lhs(acc, lhs, load_staged_rhs=waiting[unit].pop(0))

    barrier = pltpu.get_barrier_semaphore()
    for o in range(1, owners):
        pl.semaphore_signal(
            barrier,
            inc=1,
            device_id={"section": section, "expert": lax.rem(me + o, owners)},
            device_id_type=pl.DeviceIdType.MESH,
        )
    for o in range(owners):
        pl.semaphore_signal(
            barrier,
            inc=1,
            device_id={"section": 1 - section, "expert": lax.rem(me + o, owners)},
            device_id_type=pl.DeviceIdType.MESH,
        )
    tok_copies = [
        pltpu.make_async_copy(
            tok_hbm.at[m], tok_v.at[pl.ds(m * tok_rows, tok_rows)], tok_sem.at[m]
        )
        for m in range(micro)
    ]
    small_copies = [
        pltpu.make_async_copy(chosen_hbm, chosen_ref, small_sem.at[0]),
        pltpu.make_async_copy(gain_hbm, gain_ref, small_sem.at[1]),
        pltpu.make_async_copy(router_hbm, router_ref, small_sem.at[2]),
    ]
    for c in small_copies[:1] + tok_copies + small_copies[1:]:
        c.start()
    parts = 4
    deep, half = width // parts, width // 2
    w1_copies = [
        pltpu.make_async_copy(
            w1_hbm.at[0, 0, pl.ds(k * deep, deep)], w1_v.at[pl.ds(k * deep, deep)], w1_sem
        )
        for k in range(parts)
    ]
    w2_copies = [
        pltpu.make_async_copy(
            w2_hbm.at[0, 0, :, pl.ds(k * half, half)],
            w2_v.at[:, pl.ds(k * half, half)],
            w2_sem.at[k],
        )
        for k in range(2)
    ]

    small_copies[0].wait()
    for c in w1_copies + w2_copies:
        c.start()
    id_col = jnp.full((rows, 128), -1, jnp.int32)
    code_col = jnp.full((rows, 128), -1, jnp.int32)
    item_id = jnp.full((items, 128), -1, jnp.int32)
    own_id = jnp.full((items, 128), -1, jnp.int32)
    spots = [jnp.int32(0)] * each
    for m in range(micro):
        owner_of = []
        for c in range(cap):
            r = m * cap + c
            pick = chosen_ref[0, m, 0, c]
            ident = pick + m * total
            owner = lax.div(pick, jnp.int32(tok_rows))
            slot = jnp.int32(0)
            for earlier in owner_of:
                slot = slot + jnp.where(earlier == owner, 1, 0)
            owner_of.append(owner)
            inner = m * slots + slot
            id_col = jnp.where(row_iota((rows, 128)) == r, ident, id_col)
            code_col = jnp.where(row_iota((rows, 128)) == r, owner * slots + slot, code_col)
            item_id = jnp.where(row_iota((items, 128)) == owner * each + inner, ident, item_id)
            at = jnp.where(owner == me, inner, -1)
            local = pick + (m - owner) * tok_rows
            for k in range(each):
                spots[k] = jnp.where(at == k, local, spots[k])
            own_id = jnp.where(row_iota((items, 128)) == at, ident, own_id)
    ids_send[...] = id_col
    own_ref[...] = own_id

    for c in tok_copies:
        c.wait()

    def pick_rows(first, count):
        span = tile_at(first, count)
        tf_v[:, span] = tok_v[:, span].astype(F32)
        for m in range(micro):
            for k in range(slots):
                found = tf_v[pl.ds(spots[m * slots + k], 1), span]
                pick_v[m * slots + k : m * slots + k + 1, span] = found
        rows_buf[me, :, span] = pick_v[:each, span].astype(BF16)

    def row_send(to, first, count):
        span = tile_at(first, count)
        copy_to(
            rows_buf.at[me, :, span], rows_buf.at[me, :, span], rows_ssem, rows_rsem, section, to
        ).start()

    def gathered_rows():
        all_of(rows_buf.at[pl.ds(0, owners - 1)], rows_rsem).wait()
        for p in range(owners):
            xf_v[p * each : (p + 1) * each, :] = rows_buf[p].astype(F32)

    def folded(value, start):
        for b in range(TILE // 128):
            start = start + value[:, b * 128 : (b + 1) * 128]
        return start

    def scaled_tile(act, tile, stats):
        span = tile_at(tile)
        scaled = (act * gain_ref[:, span]).astype(BF16)
        weighted = scaled.astype(F32) * router_ref[:, span].astype(F32)
        return scaled, (folded(act * act, stats[0]), folded(weighted, stats[1]))

    def closing(stats):
        inverse = lax.rsqrt(jnp.sum(stats[0], axis=-1, keepdims=True) / width + EPS)
        score = jnp.sum(stats[1], axis=-1, keepdims=True)
        gate = jax.nn.sigmoid(jnp.where(inverse > 0, score * inverse, 0.0))
        return inverse, gate

    hid = {}

    def finish(pair, inverse):
        for n in (2 * pair, 2 * pair + 1):
            value = jnp.where(inverse > 0, pltpu.matmul_pop(sums[n]) * inverse, 0.0)
            hid[n] = jax.nn.gelu(value, approximate=True).astype(BF16)

    def second_matmul(inverse, done, emit):
        pairs = hid_tiles // 2
        for t in range(in_tiles):
            if t == in_tiles // 2:
                w2_copies[1].wait()
            for i in range(pairs):
                if t == 0 and i >= done:
                    finish(i, inverse)
                for unit in range(2):
                    k = 2 * i + unit
                    multiply(outs[t % 3][unit], hid[k], w2_v[tile_at(k), tile_at(t)], unit)
            if t > 0:
                emit(t - 1)
        emit(in_tiles - 1)

    def popped(t):
        return pltpu.matmul_pop(outs[t % 3][0]) + pltpu.matmul_pop(outs[t % 3][1])

    def place(base_ref, ids_ref, value_ref, picks, first, count):
        group = 16
        for m in range(micro):
            for g in range(tok_rows // group):
                ids = row_iota((group, 128)) + (m * total + g * group) + me * tok_rows
                masks = [(ids == ids_ref[r : r + 1, :], r) for r in picks(m)]
                at = slice(m * tok_rows + g * group, m * tok_rows + (g + 1) * group)
                for b in range(first * TILE // 128, (first + count) * TILE // 128):
                    span = slice(b * 128, (b + 1) * 128)
                    added = jnp.zeros((group, 128), F32)
                    for mask, r in masks:
                        added = jnp.where(mask, value_ref[r : r + 1, span], added)
                    out_v[at, span] = (base_ref[at, span].astype(F32) + added).astype(BF16)

    def whole_picks(m):
        return range(m * cap, (m + 1) * cap)

    def slot_picks(m):
        return range(m * slots, (m + 1) * slots)

    near = in_tiles // 2
    zero = jnp.zeros((items, 128), F32)

    @pl.when(section == 0)
    def _():
        pick_rows(0, near)
        pl.semaphore_wait(barrier, 2 * owners - 1)
        row_send(peer(0), 0, near)
        pick_rows(near, in_tiles - near)
        row_send(peer(0), near, in_tiles - near)
        for k in range(1, owners - 1):
            row_send(peer(k), 0, in_tiles)
        for c in small_copies[1:]:
            c.wait()
        all_of(rows_buf.at[pl.ds(0, owners - 1)], rows_ssem).wait()
        ids_copy = copy_to(ids_send, ids_recv, misc_ssem.at[0], misc_rsem.at[0], 1, me)
        ids_copy.start()
        all_of(w1_v, w1_sem).wait()
        w2_copies[0].wait()
        for k in range(2):
            for unit in range(2):
                push(w1_v[tile_at(k), tile_at(unit)], unit)
        gathered_rows()
        early = row_iota((rows, 128)) < cap
        masks = [code_col == code for code in range(owners * slots)]
        stats = (zero, zero)
        xs = []
        for k in range(in_tiles):
            halves = []
            for b in range(TILE // 128):
                span = slice(k * TILE + b * 128, k * TILE + (b + 1) * 128)
                value = jnp.zeros((rows, 128), F32)
                for p in range(owners):
                    for s in range(slots):
                        q = p * each + s
                        both = xf_v[q : q + 1, span]
                        for m in range(1, micro):
                            after = xf_v[q + m * slots : q + m * slots + 1, span]
                            both = jnp.where(early, both, after)
                        value = jnp.where(masks[p * slots + s], both, value)
                halves.append(value)
            act = jnp.concatenate(halves, axis=1)
            act = jnp.concatenate([act, jnp.zeros((items - rows, TILE), F32)], axis=0)
            scaled, stats = scaled_tile(act, k, stats)
            xs.append(scaled)
        inverse, gate = closing(stats)
        pairs = hid_tiles // 2
        for i in range(pairs):
            for k in range(in_tiles):
                for unit in range(2):
                    n = 2 * i + unit
                    ready = i == 0 and k < 2
                    rhs = None if ready else w1_v[tile_at(k), tile_at(n)]
                    multiply(sums[n], xs[k], rhs, unit)
            if i > 0:
                finish(i - 1, inverse)

        def emit(t):
            part_send[:, tile_at(t)] = (popped(t)[:rows] * gate[:rows]).astype(BF16)
            for j, (first, count) in enumerate(send_pieces):
                if first + count - 1 == t:
                    span = tile_at(first, count)
                    for p in [peer(k) for k in range(owners - 1)] + [me]:
                        copy_to(
                            part_send.at[:, span], part_recv.at[me, :, span], part_ssem,
                            part_rsem.at[j], 1, p,
                        ).start()

        second_matmul(inverse, pairs - 1, emit)
        back = copy_to(c_v, c_recv, misc_ssem.at[1], misc_rsem.at[1], 0, me)
        back.wait_recv()
        place(tok_v, ids_send, c_recv, whole_picks, 0, in_tiles)
        all_of(part_recv, part_ssem).wait()
        ids_copy.wait_send()

    @pl.when(section != 0)
    def _():
        pick_rows(0, in_tiles)
        pl.semaphore_wait(barrier, 2 * owners - 1)
        copy_to(ids_send, ids_recv, misc_ssem.at[0], misc_rsem.at[0], 1, me).wait_recv()
        for k in range(owners - 1):
            row_send(peer(k), 0, in_tiles)
        for c in small_copies[1:]:
            c.wait()
        all_of(rows_buf.at[pl.ds(0, owners - 1)], rows_ssem).wait()
        gathered_rows()
        early = lax.rem(row_iota((items, 128)), each) < slots
        match = [
            sum((item_id == ids_recv[m * cap + c : m * cap + c + 1, :]).astype(F32) for m in range(micro))
            for c in range(cap)
        ]
        all_of(w1_v, w1_sem).wait()
        w2_copies[0].wait()
        for n in range(4):
            push(w1_v[tile_at(0), tile_at(n)], n % 2)
        stats = (zero, zero)
        for j, (first, count) in enumerate(send_pieces):
            all_of(part_recv.at[:, :, tile_at(first, count)], part_rsem.at[j]).wait()
            for k in range(first, first + count):
                span = tile_at(k)
                contrib = part_recv[0, :, span].astype(F32)
                for p in range(1, owners):
                    contrib = contrib + part_recv[p, :, span].astype(F32)
                c_v[:, span] = contrib
                halves = []
                for b in range(TILE // 128):
                    inner = slice(k * TILE + b * 128, k * TILE + (b + 1) * 128)
                    act = xf_v[:, inner]
                    for c in range(cap):
                        both = c_v[c : c + 1, inner]
                        for m in range(1, micro):
                            both = jnp.where(early, both, c_v[m * cap + c : m * cap + c + 1, inner])
                        act = act + match[c] * both
                    halves.append(act.astype(BF16).astype(F32))
                scaled, stats = scaled_tile(jnp.concatenate(halves, axis=1), k, stats)
                for n in range(hid_tiles):
                    multiply(sums[n], scaled, None if n < 4 else w1_v[span, tile_at(n)], n % 2)
                if k + 1 < in_tiles:
                    for n in range(4):
                        push(w1_v[tile_at(k + 1), tile_at(n)], n % 2)
        back = copy_to(c_v, c_recv, misc_ssem.at[1], misc_rsem.at[1], 0, me)
        back.start()
        inverse, gate = closing(stats)

        def emit(t):
            value = popped(t) * gate
            for p in range(owners):
                last_send[p, :, tile_at(t)] = value[p * each : (p + 1) * each].astype(BF16)
            for j, (first, count) in enumerate(last_pieces):
                if first + count - 1 == t:
                    span = tile_at(first, count)
                    for p in [peer(k) for k in range(owners - 1)]:
                        copy_to(
                            last_send.at[p, :, span], last_recv.at[me, :, span], part_ssem,
                            last_rsem.at[j], 1, p,
                        ).start()

        second_matmul(inverse, 0, emit)
        place(tok_v, ids_recv, c_v, whole_picks, 0, in_tiles)
        for j, (first, count) in enumerate(last_pieces):
            span = tile_at(first, count)
            all_of(last_recv.at[pl.ds(0, owners - 1), :, span], last_rsem.at[j]).wait()
            value = last_send[me, :, span].astype(F32)
            for k in range(owners - 1):
                value = value + last_recv[peer(k), :, span].astype(F32)
            fin_v[:each, span] = value
            place(out_v, own_ref, fin_v, slot_picks, first, count)
        all_of(last_recv.at[pl.ds(0, owners - 1)], part_ssem).wait()
        back.wait_send()


def scoped_kernel(dims, *refs):
    hidden, width = dims[3], dims[2]
    items = dims[4] * dims[0] * dims[6]
    dma = pltpu.SemaphoreType.DMA
    shape = (items, TILE)
    pl.run_scoped(
        lambda sums, outs, *sems: relay_kernel(dims, *refs, sums, outs, *sems),
        tuple(pltpu.ACC(n % 2)(shape, F32) for n in range(max(hidden, width) // TILE)),
        tuple((pltpu.ACC(0)(shape, F32), pltpu.ACC(1)(shape, F32)) for _ in range(3)),
        dma,
        dma((len(pieces(SEND_TILES, width // TILE)),)),
        dma((len(pieces(LAST_TILES, width // TILE)),)),
        dma((2,)),
        dma((3,)),
        dma((dims[0],)),
        dma,
        dma((2,)),
        dma,
        dma,
        dma((2,)),
    )


def fused(tokens, chosen, norm_gain, router, w_in, w_out):
    micro, tok_rows, width = tokens.shape
    owners = lax.axis_size("expert")
    cap = chosen.shape[3]
    hidden = w_in.shape[3]
    rows = micro * cap
    slots = 2 * cap // owners
    each = micro * slots
    items = owners * each
    dims = (micro, tok_rows, width, hidden, owners, cap, slots)
    vmem = pl.BlockSpec(memory_space=pltpu.VMEM)
    hbm = pl.BlockSpec(memory_space=pltpu.HBM)
    result = pl.pallas_call(
        functools.partial(scoped_kernel, dims),
        out_shape=pltpu.VMEM((micro * tok_rows, width), BF16),
        in_specs=[hbm] * 6,
        out_specs=vmem,
        scratch_shapes=[
            pltpu.SMEM((1, micro, 1, cap), jnp.int32),
            pltpu.VMEM((1, width), F32),
            pltpu.VMEM((1, width), BF16),
            pltpu.VMEM((micro * tok_rows, width), BF16),
            pltpu.VMEM((micro * tok_rows, width), F32),
            pltpu.VMEM((8, width), F32),
            pltpu.VMEM((width, hidden), BF16),
            pltpu.VMEM((hidden, width), BF16),
            pltpu.VMEM((owners, each, width), BF16),
            pltpu.VMEM((items, width), F32),
            pltpu.VMEM((rows, width), BF16),
            pltpu.VMEM((owners, rows, width), BF16),
            pltpu.VMEM((owners, each, width), BF16),
            pltpu.VMEM((owners, each, width), BF16),
            pltpu.VMEM((rows, width), F32),
            pltpu.VMEM((rows, width), F32),
            pltpu.VMEM((8, width), F32),
            pltpu.VMEM((rows, 128), jnp.int32),
            pltpu.VMEM((rows, 128), jnp.int32),
            pltpu.VMEM((items, 128), jnp.int32),
        ],
        compiler_params=pltpu.CompilerParams(
            collective_id=0, has_side_effects=True, vmem_limit_bytes=60 * 1024 * 1024
        ),
    )(tokens, chosen, norm_gain, router[:, :, 0], w_in, w_out)
    return result.reshape(1, micro, tok_rows, width)


def passed_along(value, axis, steps):
    count = lax.axis_size(axis)
    leading, last = (max(0, -steps), min(count, count - steps))
    return lax.ppermute(value, axis, [(source, source + steps) for source in range(leading, last)])


def moe_layer(
    current, picks_now, gain_row, router_cols, w_first, w_second, device, owners, shards_each
):
    tok_rows, width = current.shape
    experts, capacity = picks_now.shape
    slots = 2 * capacity // owners
    floats = current.astype(jnp.float32)
    inverse_rms = lax.rsqrt(jnp.mean(floats * floats, axis=-1, keepdims=True) + 1e-06)
    normed = (floats * inverse_rms * gain_row).astype(jnp.bfloat16)
    gate_all = jax.nn.sigmoid(jnp.dot(normed, router_cols, preferred_element_type=jnp.float32))
    owner_of = picks_now // tok_rows
    onehot = (owner_of[:, :, None] == jnp.arange(owners, dtype=jnp.int32)[None, None, :]).astype(
        jnp.int32
    )
    order_slot = jnp.cumsum(onehot, axis=1) - 1
    slot_of = jnp.sum(order_slot * onehot, axis=2)
    is_mine = owner_of == device
    local_idx = picks_now - device * tok_rows
    slot_hit = (
        (slot_of[:, :, None] == jnp.arange(slots, dtype=jnp.int32)[None, None, :])
        & is_mine[:, :, None]
    ).astype(jnp.float32)
    tok_hit = (
        local_idx[:, :, None] == jnp.arange(tok_rows, dtype=jnp.int32)[None, None, :]
    ).astype(jnp.float32)
    selector = jnp.einsum("xcs,xct->xst", slot_hit, tok_hit)
    flat_select = selector.reshape(experts * slots, tok_rows)
    gate_slot = jnp.einsum("xst,tx->xs", selector, gate_all, precision=lax.Precision.HIGHEST)
    dispatched = jnp.dot(
        flat_select.astype(jnp.bfloat16), normed, preferred_element_type=jnp.float32
    ).astype(jnp.bfloat16)
    outgoing = jnp.broadcast_to(
        dispatched.reshape(experts, 1, slots, width), (experts, shards_each, slots, width)
    ).reshape(owners, slots, width)
    arrived = lax.all_to_all(outgoing, "expert", split_axis=0, concat_axis=0, tiled=True)
    item_count = arrived.shape[1]
    flat_rows = arrived.reshape(-1, width)
    hidden = jax.nn.gelu(
        jnp.dot(flat_rows, w_first, preferred_element_type=jnp.float32), approximate=True
    ).astype(jnp.bfloat16)
    partial_value = jnp.dot(hidden, w_second, preferred_element_type=jnp.float32).reshape(
        owners, item_count, width
    )
    returned = lax.all_to_all(partial_value, "expert", split_axis=0, concat_axis=0, tiled=True)
    summed = returned.reshape(experts, shards_each, slots, width).sum(axis=1)
    weighted = summed * gate_slot[:, :, None]
    contrib = jnp.dot(
        flat_select.T, weighted.reshape(experts * slots, width), precision=lax.Precision.HIGHEST
    )
    return (floats + contrib).astype(jnp.bfloat16)


def fits(tokens, chosen, w_in, sections, owners):
    micro, tok_rows, width = tokens.shape
    experts, cap = chosen.shape[2:]
    hidden = w_in.shape[3]
    slots = 2 * cap // owners
    whole_tiles = width % 512 == 0 and hidden % 512 == 0 and hidden <= 2048 and width <= 2048
    few = micro == 2 and micro * cap == 8 and owners * micro * slots == 16
    return (
        sections == 2 and experts == 1 and whole_tiles and few
        and tok_rows % 16 == 0 and micro * tok_rows <= TILE
    )


def local(tokens, chosen, norm_gain, router, w_in, w_out):
    sections = lax.axis_size("section")
    owners = lax.axis_size("expert")
    if fits(tokens, chosen, w_in, sections, owners):
        return fused(tokens, chosen, norm_gain, router, w_in, w_out)
    section_index = lax.axis_index("section")
    device = lax.axis_index("expert")
    micro_count, tok_rows, width = tokens.shape
    experts = chosen.shape[2]
    shards_each = owners // experts
    gain_row = norm_gain[0]
    router_cols = router[0]
    w_first = w_in[0, 0]
    w_second = w_out[0, 0]
    outputs = jnp.zeros((1, micro_count, tok_rows, width), jnp.bfloat16)
    received = jnp.zeros((tok_rows, width), jnp.bfloat16)
    tick_count = micro_count + sections - 1
    for tick_index in range(tick_count):
        batch_index = tick_index - section_index
        clipped = jnp.clip(batch_index, 0, micro_count - 1)
        fresh_input = tokens[min(tick_index, micro_count - 1)]
        current = jnp.where(section_index == 0, fresh_input, received)
        picks_now = lax.dynamic_index_in_dim(chosen[0], clipped, 0, keepdims=False)
        layer_out = moe_layer(
            current,
            picks_now,
            gain_row,
            router_cols,
            w_first,
            w_second,
            device,
            owners,
            shards_each,
        )
        in_range = (batch_index >= 0) & (batch_index < micro_count)
        previous = lax.dynamic_index_in_dim(outputs[0], clipped, 0, keepdims=False)
        written = jnp.where(in_range, layer_out, previous)
        outputs = lax.dynamic_update_index_in_dim(outputs, written[None, None], clipped, 1)
        if tick_index + 1 < tick_count:
            received = passed_along(layer_out, "section", 1)
    return outputs


def solution(mesh):
    placed = (
        P("group", "expert", None),
        P("section", "group", None, None),
        P("section", None),
        P("section", None, None),
        P("section", "expert", None, None),
        P("section", "expert", None, None),
    )
    return jax.shard_map(
        local,
        mesh=mesh,
        in_specs=placed,
        out_specs=P("section", "group", "expert", None),
        check_vma=False,
    )
```

```python
import functools

import jax
import jax.numpy as jnp
from jax import lax
from jax.experimental import pallas as pl
from jax.experimental.pallas import tpu as pltpu
from jax.sharding import PartitionSpec as P

F32 = jnp.float32
BF16 = jnp.bfloat16
EPS = 1e-06
TILE = 256
LAG = 2
LAST_TILES = (3, 3, 1, 1)


def row_iota(shape):
    return lax.broadcasted_iota(jnp.int32, shape, 0)


def lane_iota(shape):
    return lax.broadcasted_iota(jnp.int32, shape, 1)


def tile_at(index, count=1):
    return slice(index * TILE, (index + count) * TILE)


def pieces(sizes, tiles):
    found, start = [], 0
    for size in sizes:
        size = min(size, tiles - start)
        if size > 0:
            found.append((start, size))
            start += size
    while start < tiles:
        found.append((start, 1))
        start += 1
    return found


def relay_kernel(
    dims,
    tok_hbm,
    chosen_hbm,
    gain_hbm,
    router_hbm,
    w1_hbm,
    w2_hbm,
    out_v,
    chosen_ref,
    gain_ref,
    router_ref,
    tok_v,
    tf_v,
    pick_v,
    w1_v,
    w2_v,
    rows_buf,
    xf_v,
    part_send,
    part_recv,
    last_send,
    last_recv,
    c_v,
    c_recv,
    fin_v,
    ids_send,
    ids_recv,
    own_ref,
    sums,
    outs,
    rows_rsem,
    part_rsem,
    last_rsem,
    misc_rsem,
    small_sem,
    tok_sem,
    w1_sem,
    w2_sem,
    rows_ssem,
    part_ssem,
    misc_ssem,
):
    micro, tok_rows, width, hidden, owners, cap, slots = dims
    rows = micro * cap
    each = micro * slots
    items = owners * each
    total = owners * tok_rows
    tokens = micro * tok_rows
    in_tiles, hid_tiles = width // TILE, hidden // TILE
    send_pieces = pieces((), in_tiles)
    last_pieces = pieces(LAST_TILES, in_tiles)
    section = lax.axis_index("section")
    me = lax.axis_index("expert")

    def copy_to(src, dst, ssem, rsem, sec, exp):
        return pltpu.make_async_remote_copy(
            src_ref=src,
            dst_ref=dst,
            send_sem=ssem,
            recv_sem=rsem,
            device_id={"section": sec, "expert": exp},
            device_id_type=pl.DeviceIdType.MESH,
        )

    def all_of(ref, sem):
        return pltpu.make_async_copy(ref, ref, sem)

    def peer(k):
        low = k + jnp.where(k >= me, 1, 0)
        top = owners - 1 - k
        high = top - jnp.where(top <= me, 1, 0)
        return jnp.where(2 * me < owners, high, low)

    staged = [0, 0]

    waiting = ([], [])

    def push(rhs, unit):
        register = staged[unit]
        staged[unit] = 1 - register
        pltpu.matmul_push_rhs(rhs, staging_register=register, mxu_index=unit)
        waiting[unit].append(register)

    def multiply(acc, lhs, rhs, unit):
        if rhs is not None:
            push(rhs, unit)
        pltpu.matmul_acc_lhs(acc, lhs, load_staged_rhs=waiting[unit].pop(0))

    barrier = pltpu.get_barrier_semaphore()
    for o in range(1, owners):
        pl.semaphore_signal(
            barrier,
            inc=1,
            device_id={"section": section, "expert": lax.rem(me + o, owners)},
            device_id_type=pl.DeviceIdType.MESH,
        )
    for o in range(owners):
        pl.semaphore_signal(
            barrier,
            inc=1,
            device_id={"section": 1 - section, "expert": lax.rem(me + o, owners)},
            device_id_type=pl.DeviceIdType.MESH,
        )
    tok_copies = [
        pltpu.make_async_copy(
            tok_hbm.at[m, pl.ds(g, 8)], tok_v.at[pl.ds(m * tok_rows + g, 8)], tok_sem.at[0]
        )
        for m in range(micro)
        for g in range(0, tok_rows, 8)
    ]
    small_copies = [
        pltpu.make_async_copy(chosen_hbm, chosen_ref, small_sem.at[0]),
        pltpu.make_async_copy(gain_hbm, gain_ref, small_sem.at[1]),
        pltpu.make_async_copy(router_hbm, router_ref, small_sem.at[2]),
    ]
    for c in small_copies[:1] + tok_copies + small_copies[1:]:
        c.start()
    parts = 4
    deep, half = width // parts, width // 2
    w1_copies = [
        pltpu.make_async_copy(
            w1_hbm.at[0, 0, pl.ds(k * deep, deep)], w1_v.at[pl.ds(k * deep, deep)], w1_sem
        )
        for k in range(parts)
    ]
    w2_copies = [
        pltpu.make_async_copy(
            w2_hbm.at[0, 0, :, pl.ds(k * half, half)],
            w2_v.at[:, pl.ds(k * half, half)],
            w2_sem.at[k],
        )
        for k in range(2)
    ]

    small_copies[0].wait()
    for c in w1_copies + w2_copies:
        c.start()
    id_col = jnp.full((rows, 128), -1, jnp.int32)
    code_col = jnp.full((rows, 128), -1, jnp.int32)
    item_id = jnp.full((items, 128), -1, jnp.int32)
    own_id = jnp.full((items, 128), -1, jnp.int32)
    spots = [jnp.int32(0)] * each
    for m in range(micro):
        owner_of = []
        for c in range(cap):
            r = m * cap + c
            pick = chosen_ref[0, m, 0, c]
            ident = pick + m * total
            owner = lax.div(pick, jnp.int32(tok_rows))
            slot = jnp.int32(0)
            for earlier in owner_of:
                slot = slot + jnp.where(earlier == owner, 1, 0)
            owner_of.append(owner)
            inner = m * slots + slot
            id_col = jnp.where(row_iota((rows, 128)) == r, ident, id_col)
            code_col = jnp.where(row_iota((rows, 128)) == r, owner * slots + slot, code_col)
            item_id = jnp.where(row_iota((items, 128)) == owner * each + inner, ident, item_id)
            at = jnp.where(owner == me, inner, -1)
            local = pick + (m - owner) * tok_rows
            for k in range(each):
                spots[k] = jnp.where(at == k, local, spots[k])
            own_id = jnp.where(row_iota((items, 128)) == at, ident, own_id)
    ids_send[...] = id_col
    own_ref[...] = own_id

    all_of(tok_v.at[pl.ds(0, tokens)], tok_sem.at[0]).wait()

    def pick_rows(first, count):
        span = tile_at(first, count)
        tf_v[:, span] = tok_v[:, span].astype(F32)
        for m in range(micro):
            for k in range(slots):
                found = tf_v[pl.ds(spots[m * slots + k], 1), span]
                pick_v[m * slots + k : m * slots + k + 1, span] = found
        rows_buf[me, :, span] = pick_v[:each, span].astype(BF16)

    def row_send(to, first, count):
        span = tile_at(first, count)
        copy_to(
            rows_buf.at[me, :, span], rows_buf.at[me, :, span], rows_ssem, rows_rsem, section, to
        ).start()

    def gathered_rows():
        all_of(rows_buf.at[pl.ds(0, owners - 1)], rows_rsem).wait()
        for p in range(owners):
            xf_v[p * each : (p + 1) * each, :] = rows_buf[p].astype(F32)

    def folded(value, start):
        for b in range(TILE // 128):
            start = start + value[:, b * 128 : (b + 1) * 128]
        return start

    def scaled_tile(act, tile, stats):
        span = tile_at(tile)
        scaled = (act * gain_ref[:, span]).astype(BF16)
        weighted = scaled.astype(F32) * router_ref[:, span].astype(F32)
        return scaled, (folded(act * act, stats[0]), folded(weighted, stats[1]))

    def closing(stats):
        inverse = lax.rsqrt(jnp.sum(stats[0], axis=-1, keepdims=True) / width + EPS)
        score = jnp.sum(stats[1], axis=-1, keepdims=True)
        gate = jax.nn.sigmoid(jnp.where(inverse > 0, score * inverse, 0.0))
        return inverse, gate

    hid = {}

    def finish(pair, inverse):
        for n in (2 * pair, 2 * pair + 1):
            value = jnp.where(inverse > 0, pltpu.matmul_pop(sums[n]) * inverse, 0.0)
            hid[n] = jax.nn.gelu(value, approximate=True).astype(BF16)

    def second_matmul(inverse, done, emit):
        pairs = hid_tiles // 2
        for t in range(in_tiles):
            if t == in_tiles // 2:
                w2_copies[1].wait()
            for i in range(pairs):
                if t == 0 and i >= done:
                    finish(i, inverse)
                for unit in range(2):
                    k = 2 * i + unit
                    multiply(outs[t % 3][unit], hid[k], w2_v[tile_at(k), tile_at(t)], unit)
            if t > 0:
                emit(t - 1)
        emit(in_tiles - 1)

    def popped(t):
        return pltpu.matmul_pop(outs[t % 3][0]) + pltpu.matmul_pop(outs[t % 3][1])

    def place(base_ref, ids_ref, value_ref, picks, first, count):
        group = 16
        for m in range(micro):
            for g in range(tok_rows // group):
                ids = row_iota((group, 128)) + (m * total + g * group) + me * tok_rows
                masks = [(ids == ids_ref[r : r + 1, :], r) for r in picks(m)]
                at = slice(m * tok_rows + g * group, m * tok_rows + (g + 1) * group)
                for b in range(first * TILE // 128, (first + count) * TILE // 128):
                    span = slice(b * 128, (b + 1) * 128)
                    added = jnp.zeros((group, 128), F32)
                    for mask, r in masks:
                        added = jnp.where(mask, value_ref[r : r + 1, span], added)
                    out_v[at, span] = (base_ref[at, span].astype(F32) + added).astype(BF16)

    def whole_picks(m):
        return range(m * cap, (m + 1) * cap)

    def slot_picks(m):
        return range(m * slots, (m + 1) * slots)

    near = in_tiles // 2
    zero = jnp.zeros((items, 128), F32)

    @pl.when(section == 0)
    def _():
        pick_rows(0, near)
        pl.semaphore_wait(barrier, 2 * owners - 1)
        row_send(peer(0), 0, near)
        pick_rows(near, in_tiles - near)
        row_send(peer(0), near, in_tiles - near)
        for k in range(1, owners - 1):
            row_send(peer(k), 0, in_tiles)
        for c in small_copies[1:]:
            c.wait()
        all_of(rows_buf.at[pl.ds(0, owners - 1)], rows_ssem).wait()
        ids_copy = copy_to(ids_send, ids_recv, misc_ssem.at[0], misc_rsem.at[0], 1, me)
        ids_copy.start()
        all_of(w1_v, w1_sem).wait()
        w2_copies[0].wait()
        for k in range(2):
            for unit in range(2):
                push(w1_v[tile_at(k), tile_at(unit)], unit)
        gathered_rows()
        early = row_iota((rows, 128)) < cap
        masks = [code_col == code for code in range(owners * slots)]
        stats = (zero, zero)
        xs = []
        for k in range(in_tiles):
            halves = []
            for b in range(TILE // 128):
                span = slice(k * TILE + b * 128, k * TILE + (b + 1) * 128)
                value = jnp.zeros((rows, 128), F32)
                for p in range(owners):
                    for s in range(slots):
                        q = p * each + s
                        both = xf_v[q : q + 1, span]
                        for m in range(1, micro):
                            after = xf_v[q + m * slots : q + m * slots + 1, span]
                            both = jnp.where(early, both, after)
                        value = jnp.where(masks[p * slots + s], both, value)
                halves.append(value)
            act = jnp.concatenate(halves, axis=1)
            act = jnp.concatenate([act, jnp.zeros((items - rows, TILE), F32)], axis=0)
            scaled, stats = scaled_tile(act, k, stats)
            xs.append(scaled)
        inverse, gate = closing(stats)
        pairs = hid_tiles // 2
        for i in range(pairs):
            for k in range(in_tiles):
                for unit in range(2):
                    n = 2 * i + unit
                    ready = i == 0 and k < 2
                    rhs = None if ready else w1_v[tile_at(k), tile_at(n)]
                    multiply(sums[n], xs[k], rhs, unit)
            if i > 0:
                finish(i - 1, inverse)

        def part_start(t, to):
            span = tile_at(t)
            copy_to(
                part_send.at[:, span], part_recv.at[me, :, span], part_ssem, part_rsem.at[t], 1, to
            ).start()

        def emit(t):
            part_send[:, tile_at(t)] = (popped(t)[:rows] * gate[:rows]).astype(BF16)
            part_start(t, peer(0))
            part_start(t, me)
            for late in range(in_tiles):
                if min(late + LAG, in_tiles - 1) == t:
                    for k in range(1, owners - 1):
                        part_start(late, peer(k))

        second_matmul(inverse, pairs - 1, emit)
        back = copy_to(c_v, c_recv, misc_ssem.at[1], misc_rsem.at[1], 0, me)
        back.wait_recv()
        place(tok_v, ids_send, c_recv, whole_picks, 0, in_tiles)
        all_of(part_recv, part_ssem).wait()
        ids_copy.wait_send()

    @pl.when(section != 0)
    def _():
        pick_rows(0, in_tiles)
        pl.semaphore_wait(barrier, 2 * owners - 1)
        copy_to(ids_send, ids_recv, misc_ssem.at[0], misc_rsem.at[0], 1, me).wait_recv()
        for k in range(owners - 1):
            row_send(peer(k), 0, in_tiles)
        for c in small_copies[1:]:
            c.wait()
        all_of(rows_buf.at[pl.ds(0, owners - 1)], rows_ssem).wait()
        gathered_rows()
        early = lax.rem(row_iota((items, 128)), each) < slots
        match = [
            sum((item_id == ids_recv[m * cap + c : m * cap + c + 1, :]).astype(F32) for m in range(micro))
            for c in range(cap)
        ]
        all_of(w1_v, w1_sem).wait()
        w2_copies[0].wait()
        for n in range(2):
            push(w1_v[tile_at(0), tile_at(n)], n % 2)
        stats = (zero, zero)
        for j, (first, count) in enumerate(send_pieces):
            all_of(part_recv.at[:, :, tile_at(first, count)], part_rsem.at[j]).wait()
            for k in range(first, first + count):
                span = tile_at(k)
                contrib = part_recv[0, :, span].astype(F32)
                for p in range(1, owners):
                    contrib = contrib + part_recv[p, :, span].astype(F32)
                c_v[:, span] = contrib
                halves = []
                for b in range(TILE // 128):
                    inner = slice(k * TILE + b * 128, k * TILE + (b + 1) * 128)
                    act = xf_v[:, inner]
                    for c in range(cap):
                        both = c_v[c : c + 1, inner]
                        for m in range(1, micro):
                            both = jnp.where(early, both, c_v[m * cap + c : m * cap + c + 1, inner])
                        act = act + match[c] * both
                    halves.append(act.astype(BF16).astype(F32))
                scaled, stats = scaled_tile(jnp.concatenate(halves, axis=1), k, stats)
                for n in range(hid_tiles):
                    multiply(sums[n], scaled, None if n < 2 else w1_v[span, tile_at(n)], n % 2)
                if k + 1 < in_tiles:
                    for n in range(2):
                        push(w1_v[tile_at(k + 1), tile_at(n)], n % 2)
        back = copy_to(c_v, c_recv, misc_ssem.at[1], misc_rsem.at[1], 0, me)
        back.start()
        inverse, gate = closing(stats)

        def emit(t):
            value = popped(t) * gate
            for p in range(owners):
                last_send[p, :, tile_at(t)] = value[p * each : (p + 1) * each].astype(BF16)
            for j, (first, count) in enumerate(last_pieces):
                if first + count - 1 == t:
                    span = tile_at(first, count)
                    for p in [peer(k) for k in range(owners - 1)]:
                        copy_to(
                            last_send.at[p, :, span], last_recv.at[me, :, span], part_ssem,
                            last_rsem.at[j], 1, p,
                        ).start()

        second_matmul(inverse, 0, emit)
        place(tok_v, ids_recv, c_v, whole_picks, 0, in_tiles)
        for j, (first, count) in enumerate(last_pieces):
            span = tile_at(first, count)
            all_of(last_recv.at[pl.ds(0, owners - 1), :, span], last_rsem.at[j]).wait()
            value = last_send[me, :, span].astype(F32)
            for k in range(owners - 1):
                value = value + last_recv[peer(k), :, span].astype(F32)
            fin_v[:each, span] = value
            place(out_v, own_ref, fin_v, slot_picks, first, count)
        all_of(last_recv.at[pl.ds(0, owners - 1)], part_ssem).wait()
        back.wait_send()


def scoped_kernel(dims, *refs):
    hidden, width = dims[3], dims[2]
    items = dims[4] * dims[0] * dims[6]
    dma = pltpu.SemaphoreType.DMA
    shape = (items, TILE)
    pl.run_scoped(
        lambda sums, outs, *sems: relay_kernel(dims, *refs, sums, outs, *sems),
        tuple(pltpu.ACC(n % 2)(shape, F32) for n in range(max(hidden, width) // TILE)),
        tuple((pltpu.ACC(0)(shape, F32), pltpu.ACC(1)(shape, F32)) for _ in range(3)),
        dma,
        dma((width // TILE,)),
        dma((len(pieces(LAST_TILES, width // TILE)),)),
        dma((2,)),
        dma((3,)),
        dma((dims[0],)),
        dma,
        dma((2,)),
        dma,
        dma,
        dma((2,)),
    )


def fused(tokens, chosen, norm_gain, router, w_in, w_out):
    micro, tok_rows, width = tokens.shape
    owners = lax.axis_size("expert")
    cap = chosen.shape[3]
    hidden = w_in.shape[3]
    rows = micro * cap
    slots = 2 * cap // owners
    each = micro * slots
    items = owners * each
    dims = (micro, tok_rows, width, hidden, owners, cap, slots)
    vmem = pl.BlockSpec(memory_space=pltpu.VMEM)
    hbm = pl.BlockSpec(memory_space=pltpu.HBM)
    result = pl.pallas_call(
        functools.partial(scoped_kernel, dims),
        out_shape=pltpu.VMEM((micro * tok_rows, width), BF16),
        in_specs=[hbm] * 6,
        out_specs=vmem,
        scratch_shapes=[
            pltpu.SMEM((1, micro, 1, cap), jnp.int32),
            pltpu.VMEM((1, width), F32),
            pltpu.VMEM((1, width), BF16),
            pltpu.VMEM((micro * tok_rows, width), BF16),
            pltpu.VMEM((micro * tok_rows, width), F32),
            pltpu.VMEM((8, width), F32),
            pltpu.VMEM((width, hidden), BF16),
            pltpu.VMEM((hidden, width), BF16),
            pltpu.VMEM((owners, each, width), BF16),
            pltpu.VMEM((items, width), F32),
            pltpu.VMEM((rows, width), BF16),
            pltpu.VMEM((owners, rows, width), BF16),
            pltpu.VMEM((owners, each, width), BF16),
            pltpu.VMEM((owners, each, width), BF16),
            pltpu.VMEM((rows, width), F32),
            pltpu.VMEM((rows, width), F32),
            pltpu.VMEM((8, width), F32),
            pltpu.VMEM((rows, 128), jnp.int32),
            pltpu.VMEM((rows, 128), jnp.int32),
            pltpu.VMEM((items, 128), jnp.int32),
        ],
        compiler_params=pltpu.CompilerParams(
            collective_id=0, has_side_effects=True, vmem_limit_bytes=60 * 1024 * 1024
        ),
    )(tokens, chosen, norm_gain, router[:, :, 0], w_in, w_out)
    return result.reshape(1, micro, tok_rows, width)


def passed_along(value, axis, steps):
    count = lax.axis_size(axis)
    leading, last = (max(0, -steps), min(count, count - steps))
    return lax.ppermute(value, axis, [(source, source + steps) for source in range(leading, last)])


def moe_layer(
    current, picks_now, gain_row, router_cols, w_first, w_second, device, owners, shards_each
):
    tok_rows, width = current.shape
    experts, capacity = picks_now.shape
    slots = 2 * capacity // owners
    floats = current.astype(jnp.float32)
    inverse_rms = lax.rsqrt(jnp.mean(floats * floats, axis=-1, keepdims=True) + 1e-06)
    normed = (floats * inverse_rms * gain_row).astype(jnp.bfloat16)
    gate_all = jax.nn.sigmoid(jnp.dot(normed, router_cols, preferred_element_type=jnp.float32))
    owner_of = picks_now // tok_rows
    onehot = (owner_of[:, :, None] == jnp.arange(owners, dtype=jnp.int32)[None, None, :]).astype(
        jnp.int32
    )
    order_slot = jnp.cumsum(onehot, axis=1) - 1
    slot_of = jnp.sum(order_slot * onehot, axis=2)
    is_mine = owner_of == device
    local_idx = picks_now - device * tok_rows
    slot_hit = (
        (slot_of[:, :, None] == jnp.arange(slots, dtype=jnp.int32)[None, None, :])
        & is_mine[:, :, None]
    ).astype(jnp.float32)
    tok_hit = (
        local_idx[:, :, None] == jnp.arange(tok_rows, dtype=jnp.int32)[None, None, :]
    ).astype(jnp.float32)
    selector = jnp.einsum("xcs,xct->xst", slot_hit, tok_hit)
    flat_select = selector.reshape(experts * slots, tok_rows)
    gate_slot = jnp.einsum("xst,tx->xs", selector, gate_all, precision=lax.Precision.HIGHEST)
    dispatched = jnp.dot(
        flat_select.astype(jnp.bfloat16), normed, preferred_element_type=jnp.float32
    ).astype(jnp.bfloat16)
    outgoing = jnp.broadcast_to(
        dispatched.reshape(experts, 1, slots, width), (experts, shards_each, slots, width)
    ).reshape(owners, slots, width)
    arrived = lax.all_to_all(outgoing, "expert", split_axis=0, concat_axis=0, tiled=True)
    item_count = arrived.shape[1]
    flat_rows = arrived.reshape(-1, width)
    hidden = jax.nn.gelu(
        jnp.dot(flat_rows, w_first, preferred_element_type=jnp.float32), approximate=True
    ).astype(jnp.bfloat16)
    partial_value = jnp.dot(hidden, w_second, preferred_element_type=jnp.float32).reshape(
        owners, item_count, width
    )
    returned = lax.all_to_all(partial_value, "expert", split_axis=0, concat_axis=0, tiled=True)
    summed = returned.reshape(experts, shards_each, slots, width).sum(axis=1)
    weighted = summed * gate_slot[:, :, None]
    contrib = jnp.dot(
        flat_select.T, weighted.reshape(experts * slots, width), precision=lax.Precision.HIGHEST
    )
    return (floats + contrib).astype(jnp.bfloat16)


def fits(tokens, chosen, w_in, sections, owners):
    micro, tok_rows, width = tokens.shape
    experts, cap = chosen.shape[2:]
    hidden = w_in.shape[3]
    slots = 2 * cap // owners
    whole_tiles = width % 512 == 0 and hidden % 512 == 0 and hidden <= 2048 and width <= 2048
    few = micro == 2 and micro * cap == 8 and owners * micro * slots == 16
    return (
        sections == 2 and experts == 1 and whole_tiles and few
        and tok_rows % 16 == 0 and micro * tok_rows <= TILE
    )


def local(tokens, chosen, norm_gain, router, w_in, w_out):
    sections = lax.axis_size("section")
    owners = lax.axis_size("expert")
    if fits(tokens, chosen, w_in, sections, owners):
        return fused(tokens, chosen, norm_gain, router, w_in, w_out)
    section_index = lax.axis_index("section")
    device = lax.axis_index("expert")
    micro_count, tok_rows, width = tokens.shape
    experts = chosen.shape[2]
    shards_each = owners // experts
    gain_row = norm_gain[0]
    router_cols = router[0]
    w_first = w_in[0, 0]
    w_second = w_out[0, 0]
    outputs = jnp.zeros((1, micro_count, tok_rows, width), jnp.bfloat16)
    received = jnp.zeros((tok_rows, width), jnp.bfloat16)
    tick_count = micro_count + sections - 1
    for tick_index in range(tick_count):
        batch_index = tick_index - section_index
        clipped = jnp.clip(batch_index, 0, micro_count - 1)
        fresh_input = tokens[min(tick_index, micro_count - 1)]
        current = jnp.where(section_index == 0, fresh_input, received)
        picks_now = lax.dynamic_index_in_dim(chosen[0], clipped, 0, keepdims=False)
        layer_out = moe_layer(
            current,
            picks_now,
            gain_row,
            router_cols,
            w_first,
            w_second,
            device,
            owners,
            shards_each,
        )
        in_range = (batch_index >= 0) & (batch_index < micro_count)
        previous = lax.dynamic_index_in_dim(outputs[0], clipped, 0, keepdims=False)
        written = jnp.where(in_range, layer_out, previous)
        outputs = lax.dynamic_update_index_in_dim(outputs, written[None, None], clipped, 1)
        if tick_index + 1 < tick_count:
            received = passed_along(layer_out, "section", 1)
    return outputs


def solution(mesh):
    placed = (
        P("group", "expert", None),
        P("section", "group", None, None),
        P("section", None),
        P("section", None, None),
        P("section", "expert", None, None),
        P("section", "expert", None, None),
    )
    return jax.shard_map(
        local,
        mesh=mesh,
        in_specs=placed,
        out_specs=P("section", "group", "expert", None),
        check_vma=False,
    )
```

```python
import functools

import jax
import jax.numpy as jnp
from jax import lax
from jax.experimental import pallas as pl
from jax.experimental.pallas import tpu as pltpu
from jax.sharding import PartitionSpec as P

F32 = jnp.float32
BF16 = jnp.bfloat16
EPS = 1e-06
TILE = 256
LAG = 2
LAST_TILES = (3, 3, 1, 1)


def row_iota(shape):
    return lax.broadcasted_iota(jnp.int32, shape, 0)


def lane_iota(shape):
    return lax.broadcasted_iota(jnp.int32, shape, 1)


def tile_at(index, count=1):
    return slice(index * TILE, (index + count) * TILE)


def pieces(sizes, tiles):
    found, start = [], 0
    for size in sizes:
        size = min(size, tiles - start)
        if size > 0:
            found.append((start, size))
            start += size
    while start < tiles:
        found.append((start, 1))
        start += 1
    return found


def relay_kernel(
    dims,
    tok_hbm,
    chosen_hbm,
    gain_hbm,
    router_hbm,
    w1_hbm,
    w2_hbm,
    out_v,
    chosen_ref,
    gain_ref,
    router_ref,
    tok_v,
    tf_v,
    pick_v,
    w1_v,
    w2_v,
    rows_buf,
    xf_v,
    part_send,
    part_recv,
    last_send,
    last_recv,
    c_v,
    c_recv,
    fin_v,
    ids_send,
    ids_recv,
    own_ref,
    sums,
    outs,
    rows_rsem,
    part_rsem,
    last_rsem,
    misc_rsem,
    small_sem,
    tok_sem,
    w1_sem,
    w2_sem,
    rows_ssem,
    part_ssem,
    misc_ssem,
):
    micro, tok_rows, width, hidden, owners, cap, slots = dims
    rows = micro * cap
    each = micro * slots
    items = owners * each
    total = owners * tok_rows
    tokens = micro * tok_rows
    in_tiles, hid_tiles = width // TILE, hidden // TILE
    send_pieces = pieces((), in_tiles)
    last_pieces = pieces(LAST_TILES, in_tiles)
    section = lax.axis_index("section")
    me = lax.axis_index("expert")

    def copy_to(src, dst, ssem, rsem, sec, exp):
        return pltpu.make_async_remote_copy(
            src_ref=src,
            dst_ref=dst,
            send_sem=ssem,
            recv_sem=rsem,
            device_id={"section": sec, "expert": exp},
            device_id_type=pl.DeviceIdType.MESH,
        )

    def all_of(ref, sem):
        return pltpu.make_async_copy(ref, ref, sem)

    def peer(k):
        low = k + jnp.where(k >= me, 1, 0)
        top = owners - 1 - k
        high = top - jnp.where(top <= me, 1, 0)
        return jnp.where(2 * me < owners, high, low)

    staged = [0, 0]

    waiting = ([], [])

    def push(rhs, unit):
        register = staged[unit]
        staged[unit] = 1 - register
        pltpu.matmul_push_rhs(rhs, staging_register=register, mxu_index=unit)
        waiting[unit].append(register)

    def multiply(acc, lhs, rhs, unit):
        if rhs is not None:
            push(rhs, unit)
        pltpu.matmul_acc_lhs(acc, lhs, load_staged_rhs=waiting[unit].pop(0))

    barrier = pltpu.get_barrier_semaphore()
    for o in range(1, owners):
        pl.semaphore_signal(
            barrier,
            inc=1,
            device_id={"section": section, "expert": lax.rem(me + o, owners)},
            device_id_type=pl.DeviceIdType.MESH,
        )
    for o in range(owners):
        pl.semaphore_signal(
            barrier,
            inc=1,
            device_id={"section": 1 - section, "expert": lax.rem(me + o, owners)},
            device_id_type=pl.DeviceIdType.MESH,
        )
    tok_copies = [
        pltpu.make_async_copy(
            tok_hbm.at[m, pl.ds(g, 8)], tok_v.at[pl.ds(m * tok_rows + g, 8)], tok_sem.at[0]
        )
        for m in range(micro)
        for g in range(0, tok_rows, 8)
    ]
    small_copies = [
        pltpu.make_async_copy(chosen_hbm, chosen_ref, small_sem.at[0]),
        pltpu.make_async_copy(gain_hbm, gain_ref, small_sem.at[1]),
        pltpu.make_async_copy(router_hbm, router_ref, small_sem.at[2]),
    ]
    for c in small_copies[:1] + tok_copies + small_copies[1:]:
        c.start()
    parts = 4
    deep, half = width // parts, width // 2
    w1_copies = [
        pltpu.make_async_copy(
            w1_hbm.at[0, 0, pl.ds(k * deep, deep)], w1_v.at[pl.ds(k * deep, deep)], w1_sem
        )
        for k in range(parts)
    ]
    w2_copies = [
        pltpu.make_async_copy(
            w2_hbm.at[0, 0, :, pl.ds(k * half, half)],
            w2_v.at[:, pl.ds(k * half, half)],
            w2_sem.at[k],
        )
        for k in range(2)
    ]

    small_copies[0].wait()
    for c in w1_copies + w2_copies:
        c.start()
    id_col = jnp.full((rows, 128), -1, jnp.int32)
    code_col = jnp.full((rows, 128), -1, jnp.int32)
    item_id = jnp.full((items, 128), -1, jnp.int32)
    own_id = jnp.full((items, 128), -1, jnp.int32)
    spots = [jnp.int32(0)] * each
    for m in range(micro):
        owner_of = []
        for c in range(cap):
            r = m * cap + c
            pick = chosen_ref[0, m, 0, c]
            ident = pick + m * total
            owner = lax.div(pick, jnp.int32(tok_rows))
            slot = jnp.int32(0)
            for earlier in owner_of:
                slot = slot + jnp.where(earlier == owner, 1, 0)
            owner_of.append(owner)
            inner = m * slots + slot
            id_col = jnp.where(row_iota((rows, 128)) == r, ident, id_col)
            code_col = jnp.where(row_iota((rows, 128)) == r, owner * slots + slot, code_col)
            item_id = jnp.where(row_iota((items, 128)) == owner * each + inner, ident, item_id)
            at = jnp.where(owner == me, inner, -1)
            local = pick + (m - owner) * tok_rows
            for k in range(each):
                spots[k] = jnp.where(at == k, local, spots[k])
            own_id = jnp.where(row_iota((items, 128)) == at, ident, own_id)
    ids_send[...] = id_col
    own_ref[...] = own_id

    all_of(tok_v.at[pl.ds(0, tokens)], tok_sem.at[0]).wait()

    def pick_rows(first, count):
        span = tile_at(first, count)
        tf_v[:, span] = tok_v[:, span].astype(F32)
        for m in range(micro):
            for k in range(slots):
                found = tf_v[pl.ds(spots[m * slots + k], 1), span]
                pick_v[m * slots + k : m * slots + k + 1, span] = found
        rows_buf[me, :, span] = pick_v[:each, span].astype(BF16)

    def row_send(to, first, count):
        span = tile_at(first, count)
        copy_to(
            rows_buf.at[me, :, span], rows_buf.at[me, :, span], rows_ssem, rows_rsem.at[me], section, to
        ).start()

    def gathered_rows():
        for k in range(owners - 1):
            all_of(rows_buf.at[peer(k)], rows_rsem.at[peer(k)]).wait()
        for p in range(owners):
            xf_v[p * each : (p + 1) * each, :] = rows_buf[p].astype(F32)

    def folded(value, start):
        for b in range(TILE // 128):
            start = start + value[:, b * 128 : (b + 1) * 128]
        return start

    def scaled_tile(act, tile, stats):
        span = tile_at(tile)
        scaled = (act * gain_ref[:, span]).astype(BF16)
        weighted = scaled.astype(F32) * router_ref[:, span].astype(F32)
        return scaled, (folded(act * act, stats[0]), folded(weighted, stats[1]))

    def closing(stats):
        inverse = lax.rsqrt(jnp.sum(stats[0], axis=-1, keepdims=True) / width + EPS)
        score = jnp.sum(stats[1], axis=-1, keepdims=True)
        gate = jax.nn.sigmoid(jnp.where(inverse > 0, score * inverse, 0.0))
        return inverse, gate

    hid = {}

    def finish(pair, inverse):
        for n in (2 * pair, 2 * pair + 1):
            value = jnp.where(inverse > 0, pltpu.matmul_pop(sums[n]) * inverse, 0.0)
            hid[n] = jax.nn.gelu(value, approximate=True).astype(BF16)

    def second_matmul(inverse, done, emit):
        pairs = hid_tiles // 2
        for t in range(in_tiles):
            if t == in_tiles // 2:
                w2_copies[1].wait()
            for i in range(pairs):
                if t == 0 and i >= done:
                    finish(i, inverse)
                for unit in range(2):
                    k = 2 * i + unit
                    multiply(outs[t % 3][unit], hid[k], w2_v[tile_at(k), tile_at(t)], unit)
            if t > 0:
                emit(t - 1)
        emit(in_tiles - 1)

    def popped(t):
        return pltpu.matmul_pop(outs[t % 3][0]) + pltpu.matmul_pop(outs[t % 3][1])

    def place(base_ref, ids_ref, value_ref, picks, first, count):
        group = 16
        for m in range(micro):
            for g in range(tok_rows // group):
                ids = row_iota((group, 128)) + (m * total + g * group) + me * tok_rows
                masks = [(ids == ids_ref[r : r + 1, :], r) for r in picks(m)]
                at = slice(m * tok_rows + g * group, m * tok_rows + (g + 1) * group)
                for b in range(first * TILE // 128, (first + count) * TILE // 128):
                    span = slice(b * 128, (b + 1) * 128)
                    added = jnp.zeros((group, 128), F32)
                    for mask, r in masks:
                        added = jnp.where(mask, value_ref[r : r + 1, span], added)
                    out_v[at, span] = (base_ref[at, span].astype(F32) + added).astype(BF16)

    def whole_picks(m):
        return range(m * cap, (m + 1) * cap)

    def slot_picks(m):
        return range(m * slots, (m + 1) * slots)

    zero = jnp.zeros((items, 128), F32)

    @pl.when(section == 0)
    def _():
        pick_rows(0, in_tiles)
        pl.semaphore_wait(barrier, 2 * owners - 1)
        row_send(peer(0), 0, in_tiles)
        for k in range(1, owners - 1):
            row_send(peer(k), 0, in_tiles)
        for c in small_copies[1:]:
            c.wait()
        all_of(rows_buf.at[pl.ds(0, owners - 1)], rows_ssem).wait()
        ids_copy = copy_to(ids_send, ids_recv, misc_ssem.at[0], misc_rsem.at[0], 1, me)
        ids_copy.start()
        all_of(w1_v, w1_sem).wait()
        w2_copies[0].wait()
        for k in range(2):
            for unit in range(2):
                push(w1_v[tile_at(k), tile_at(unit)], unit)
        early = row_iota((rows, 128)) < cap

        def chosen_rows(value, j, owner, span):
            for s in range(slots):
                q = j * each + s
                both = xf_v[q : q + 1, span]
                for m in range(1, micro):
                    after = xf_v[q + m * slots : q + m * slots + 1, span]
                    both = jnp.where(early, both, after)
                value = jnp.where(code_col == owner * slots + s, both, value)
            return value

        spans = [slice(b * 128, (b + 1) * 128) for b in range(width // 128)]
        order = [me] + [peer(owners - 2 - k) for k in range(owners - 1)]
        for j, owner in enumerate(order):
            if j > 0:
                all_of(rows_buf.at[owner], rows_rsem.at[owner]).wait()
            xf_v[j * each : (j + 1) * each, :] = rows_buf[owner].astype(F32)
            if j + 1 < owners:
                for span in spans:
                    start = c_v[:, span] if j > 0 else jnp.zeros((rows, 128), F32)
                    c_v[:, span] = chosen_rows(start, j, owner, span)
        stats = (zero, zero)
        xs = []
        for k in range(in_tiles):
            act = jnp.concatenate(
                [
                    chosen_rows(c_v[:, span], owners - 1, order[-1], span)
                    for span in spans[k * TILE // 128 : (k + 1) * TILE // 128]
                ],
                axis=1,
            )
            act = jnp.concatenate([act, jnp.zeros((items - rows, TILE), F32)], axis=0)
            scaled, stats = scaled_tile(act, k, stats)
            xs.append(scaled)
        inverse, gate = closing(stats)
        pairs = hid_tiles // 2
        for i in range(pairs):
            for k in range(in_tiles):
                for unit in range(2):
                    n = 2 * i + unit
                    ready = i == 0 and k < 2
                    rhs = None if ready else w1_v[tile_at(k), tile_at(n)]
                    multiply(sums[n], xs[k], rhs, unit)
            if i > 0:
                finish(i - 1, inverse)

        def part_start(t, to):
            span = tile_at(t)
            copy_to(
                part_send.at[:, span], part_recv.at[me, :, span], part_ssem, part_rsem.at[t], 1, to
            ).start()

        def emit(t):
            part_send[:, tile_at(t)] = (popped(t)[:rows] * gate[:rows]).astype(BF16)
            part_start(t, peer(0))
            part_start(t, me)
            for late in range(in_tiles):
                if min(late + LAG, in_tiles - 1) == t:
                    for k in range(1, owners - 1):
                        part_start(late, peer(k))

        second_matmul(inverse, pairs - 1, emit)
        back = copy_to(c_v, c_recv, misc_ssem.at[1], misc_rsem.at[1], 0, me)
        back.wait_recv()
        place(tok_v, ids_send, c_recv, whole_picks, 0, in_tiles)
        all_of(part_recv, part_ssem).wait()
        ids_copy.wait_send()

    @pl.when(section != 0)
    def _():
        pick_rows(0, in_tiles)
        pl.semaphore_wait(barrier, 2 * owners - 1)
        copy_to(ids_send, ids_recv, misc_ssem.at[0], misc_rsem.at[0], 1, me).wait_recv()
        for k in range(owners - 1):
            row_send(peer(k), 0, in_tiles)
        for c in small_copies[1:]:
            c.wait()
        all_of(rows_buf.at[pl.ds(0, owners - 1)], rows_ssem).wait()
        gathered_rows()
        early = lax.rem(row_iota((items, 128)), each) < slots
        match = [
            sum((item_id == ids_recv[m * cap + c : m * cap + c + 1, :]).astype(F32) for m in range(micro))
            for c in range(cap)
        ]
        all_of(w1_v, w1_sem).wait()
        w2_copies[0].wait()
        for n in range(2):
            push(w1_v[tile_at(0), tile_at(n)], n % 2)
        stats = (zero, zero)
        for j, (first, count) in enumerate(send_pieces):
            all_of(part_recv.at[:, :, tile_at(first, count)], part_rsem.at[j]).wait()
            for k in range(first, first + count):
                span = tile_at(k)
                contrib = part_recv[0, :, span].astype(F32)
                for p in range(1, owners):
                    contrib = contrib + part_recv[p, :, span].astype(F32)
                c_v[:, span] = contrib
                halves = []
                for b in range(TILE // 128):
                    inner = slice(k * TILE + b * 128, k * TILE + (b + 1) * 128)
                    act = xf_v[:, inner]
                    for c in range(cap):
                        both = c_v[c : c + 1, inner]
                        for m in range(1, micro):
                            both = jnp.where(early, both, c_v[m * cap + c : m * cap + c + 1, inner])
                        act = act + match[c] * both
                    halves.append(act.astype(BF16).astype(F32))
                scaled, stats = scaled_tile(jnp.concatenate(halves, axis=1), k, stats)
                for n in range(hid_tiles):
                    multiply(sums[n], scaled, None if n < 2 else w1_v[span, tile_at(n)], n % 2)
                if k + 1 < in_tiles:
                    for n in range(2):
                        push(w1_v[tile_at(k + 1), tile_at(n)], n % 2)
        back = copy_to(c_v, c_recv, misc_ssem.at[1], misc_rsem.at[1], 0, me)
        back.start()
        inverse, gate = closing(stats)

        def emit(t):
            value = popped(t) * gate
            for p in range(owners):
                last_send[p, :, tile_at(t)] = value[p * each : (p + 1) * each].astype(BF16)
            for j, (first, count) in enumerate(last_pieces):
                if first + count - 1 == t:
                    span = tile_at(first, count)
                    for p in [peer(k) for k in range(owners - 1)]:
                        copy_to(
                            last_send.at[p, :, span], last_recv.at[me, :, span], part_ssem,
                            last_rsem.at[j], 1, p,
                        ).start()

        second_matmul(inverse, 0, emit)
        place(tok_v, ids_recv, c_v, whole_picks, 0, in_tiles)
        for j, (first, count) in enumerate(last_pieces):
            span = tile_at(first, count)
            all_of(last_recv.at[pl.ds(0, owners - 1), :, span], last_rsem.at[j]).wait()
            value = last_send[me, :, span].astype(F32)
            for k in range(owners - 1):
                value = value + last_recv[peer(k), :, span].astype(F32)
            fin_v[:each, span] = value
            place(out_v, own_ref, fin_v, slot_picks, first, count)
        all_of(last_recv.at[pl.ds(0, owners - 1)], part_ssem).wait()
        back.wait_send()


def scoped_kernel(dims, *refs):
    hidden, width = dims[3], dims[2]
    items = dims[4] * dims[0] * dims[6]
    dma = pltpu.SemaphoreType.DMA
    shape = (items, TILE)
    pl.run_scoped(
        lambda sums, outs, *sems: relay_kernel(dims, *refs, sums, outs, *sems),
        tuple(pltpu.ACC(n % 2)(shape, F32) for n in range(max(hidden, width) // TILE)),
        tuple((pltpu.ACC(0)(shape, F32), pltpu.ACC(1)(shape, F32)) for _ in range(3)),
        dma((dims[4],)),
        dma((width // TILE,)),
        dma((len(pieces(LAST_TILES, width // TILE)),)),
        dma((2,)),
        dma((3,)),
        dma((dims[0],)),
        dma,
        dma((2,)),
        dma,
        dma,
        dma((2,)),
    )


def fused(tokens, chosen, norm_gain, router, w_in, w_out):
    micro, tok_rows, width = tokens.shape
    owners = lax.axis_size("expert")
    cap = chosen.shape[3]
    hidden = w_in.shape[3]
    rows = micro * cap
    slots = 2 * cap // owners
    each = micro * slots
    items = owners * each
    dims = (micro, tok_rows, width, hidden, owners, cap, slots)
    vmem = pl.BlockSpec(memory_space=pltpu.VMEM)
    hbm = pl.BlockSpec(memory_space=pltpu.HBM)
    result = pl.pallas_call(
        functools.partial(scoped_kernel, dims),
        out_shape=pltpu.VMEM((micro * tok_rows, width), BF16),
        in_specs=[hbm] * 6,
        out_specs=vmem,
        scratch_shapes=[
            pltpu.SMEM((1, micro, 1, cap), jnp.int32),
            pltpu.VMEM((1, width), F32),
            pltpu.VMEM((1, width), BF16),
            pltpu.VMEM((micro * tok_rows, width), BF16),
            pltpu.VMEM((micro * tok_rows, width), F32),
            pltpu.VMEM((8, width), F32),
            pltpu.VMEM((width, hidden), BF16),
            pltpu.VMEM((hidden, width), BF16),
            pltpu.VMEM((owners, each, width), BF16),
            pltpu.VMEM((items, width), F32),
            pltpu.VMEM((rows, width), BF16),
            pltpu.VMEM((owners, rows, width), BF16),
            pltpu.VMEM((owners, each, width), BF16),
            pltpu.VMEM((owners, each, width), BF16),
            pltpu.VMEM((rows, width), F32),
            pltpu.VMEM((rows, width), F32),
            pltpu.VMEM((8, width), F32),
            pltpu.VMEM((rows, 128), jnp.int32),
            pltpu.VMEM((rows, 128), jnp.int32),
            pltpu.VMEM((items, 128), jnp.int32),
        ],
        compiler_params=pltpu.CompilerParams(
            collective_id=0, has_side_effects=True, vmem_limit_bytes=60 * 1024 * 1024
        ),
    )(tokens, chosen, norm_gain, router[:, :, 0], w_in, w_out)
    return result.reshape(1, micro, tok_rows, width)


def passed_along(value, axis, steps):
    count = lax.axis_size(axis)
    leading, last = (max(0, -steps), min(count, count - steps))
    return lax.ppermute(value, axis, [(source, source + steps) for source in range(leading, last)])


def moe_layer(
    current, picks_now, gain_row, router_cols, w_first, w_second, device, owners, shards_each
):
    tok_rows, width = current.shape
    experts, capacity = picks_now.shape
    slots = 2 * capacity // owners
    floats = current.astype(jnp.float32)
    inverse_rms = lax.rsqrt(jnp.mean(floats * floats, axis=-1, keepdims=True) + 1e-06)
    normed = (floats * inverse_rms * gain_row).astype(jnp.bfloat16)
    gate_all = jax.nn.sigmoid(jnp.dot(normed, router_cols, preferred_element_type=jnp.float32))
    owner_of = picks_now // tok_rows
    onehot = (owner_of[:, :, None] == jnp.arange(owners, dtype=jnp.int32)[None, None, :]).astype(
        jnp.int32
    )
    order_slot = jnp.cumsum(onehot, axis=1) - 1
    slot_of = jnp.sum(order_slot * onehot, axis=2)
    is_mine = owner_of == device
    local_idx = picks_now - device * tok_rows
    slot_hit = (
        (slot_of[:, :, None] == jnp.arange(slots, dtype=jnp.int32)[None, None, :])
        & is_mine[:, :, None]
    ).astype(jnp.float32)
    tok_hit = (
        local_idx[:, :, None] == jnp.arange(tok_rows, dtype=jnp.int32)[None, None, :]
    ).astype(jnp.float32)
    selector = jnp.einsum("xcs,xct->xst", slot_hit, tok_hit)
    flat_select = selector.reshape(experts * slots, tok_rows)
    gate_slot = jnp.einsum("xst,tx->xs", selector, gate_all, precision=lax.Precision.HIGHEST)
    dispatched = jnp.dot(
        flat_select.astype(jnp.bfloat16), normed, preferred_element_type=jnp.float32
    ).astype(jnp.bfloat16)
    outgoing = jnp.broadcast_to(
        dispatched.reshape(experts, 1, slots, width), (experts, shards_each, slots, width)
    ).reshape(owners, slots, width)
    arrived = lax.all_to_all(outgoing, "expert", split_axis=0, concat_axis=0, tiled=True)
    item_count = arrived.shape[1]
    flat_rows = arrived.reshape(-1, width)
    hidden = jax.nn.gelu(
        jnp.dot(flat_rows, w_first, preferred_element_type=jnp.float32), approximate=True
    ).astype(jnp.bfloat16)
    partial_value = jnp.dot(hidden, w_second, preferred_element_type=jnp.float32).reshape(
        owners, item_count, width
    )
    returned = lax.all_to_all(partial_value, "expert", split_axis=0, concat_axis=0, tiled=True)
    summed = returned.reshape(experts, shards_each, slots, width).sum(axis=1)
    weighted = summed * gate_slot[:, :, None]
    contrib = jnp.dot(
        flat_select.T, weighted.reshape(experts * slots, width), precision=lax.Precision.HIGHEST
    )
    return (floats + contrib).astype(jnp.bfloat16)


def fits(tokens, chosen, w_in, sections, owners):
    micro, tok_rows, width = tokens.shape
    experts, cap = chosen.shape[2:]
    hidden = w_in.shape[3]
    slots = 2 * cap // owners
    whole_tiles = width % 512 == 0 and hidden % 512 == 0 and hidden <= 2048 and width <= 2048
    few = micro == 2 and micro * cap == 8 and owners * micro * slots == 16
    return (
        sections == 2 and experts == 1 and whole_tiles and few
        and tok_rows % 16 == 0 and micro * tok_rows <= TILE
    )


def local(tokens, chosen, norm_gain, router, w_in, w_out):
    sections = lax.axis_size("section")
    owners = lax.axis_size("expert")
    if fits(tokens, chosen, w_in, sections, owners):
        return fused(tokens, chosen, norm_gain, router, w_in, w_out)
    section_index = lax.axis_index("section")
    device = lax.axis_index("expert")
    micro_count, tok_rows, width = tokens.shape
    experts = chosen.shape[2]
    shards_each = owners // experts
    gain_row = norm_gain[0]
    router_cols = router[0]
    w_first = w_in[0, 0]
    w_second = w_out[0, 0]
    outputs = jnp.zeros((1, micro_count, tok_rows, width), jnp.bfloat16)
    received = jnp.zeros((tok_rows, width), jnp.bfloat16)
    tick_count = micro_count + sections - 1
    for tick_index in range(tick_count):
        batch_index = tick_index - section_index
        clipped = jnp.clip(batch_index, 0, micro_count - 1)
        fresh_input = tokens[min(tick_index, micro_count - 1)]
        current = jnp.where(section_index == 0, fresh_input, received)
        picks_now = lax.dynamic_index_in_dim(chosen[0], clipped, 0, keepdims=False)
        layer_out = moe_layer(
            current,
            picks_now,
            gain_row,
            router_cols,
            w_first,
            w_second,
            device,
            owners,
            shards_each,
        )
        in_range = (batch_index >= 0) & (batch_index < micro_count)
        previous = lax.dynamic_index_in_dim(outputs[0], clipped, 0, keepdims=False)
        written = jnp.where(in_range, layer_out, previous)
        outputs = lax.dynamic_update_index_in_dim(outputs, written[None, None], clipped, 1)
        if tick_index + 1 < tick_count:
            received = passed_along(layer_out, "section", 1)
    return outputs


def solution(mesh):
    placed = (
        P("group", "expert", None),
        P("section", "group", None, None),
        P("section", None),
        P("section", None, None),
        P("section", "expert", None, None),
        P("section", "expert", None, None),
    )
    return jax.shard_map(
        local,
        mesh=mesh,
        in_specs=placed,
        out_specs=P("section", "group", "expert", None),
        check_vma=False,
    )
```
